256 devices in a mesh: depth: 64 (over y, x, z_hi), tile: 4 (over z_lo, core).
Axes of the slice: x: 4, y: 4, z: 8 (z_hi: 4, z_lo: 2; z = z_hi * 2 + z_lo), core: 2. Of those that a mesh axis runs over, the one named last changes fastest.
Arguments:
- coarse: bfloat16 [128, 256, 256], P('depth', None, 'tile'), may hold values from -6 to 6
- residual: bfloat16 [256, 512, 512], P('depth', None, 'tile'), may hold values from -6 to 6
- levels: int32 [64, 128, 128], P('depth', None, 'tile'), may hold values from 0 to 2
- slab_rank: int32 [64], replicated, may hold values from -64 to 63, as said below
- light_angles: float32 [2], replicated, may hold values from -3.140625 to 3.140625
- color_slope: float32 [3], replicated, may hold values from 0.5 to 2
- color_shift: float32 [3], replicated, may hold values from -1 to 1
Outputs:
- image: float32 [4, 512, 512], P(None, 'depth', 'tile')
- slab_shade: float32 [64, 512, 512], P('depth', None, 'tile')
The draws below stay inside these ranges and needn't reach their ends.
Inputs may be any that keep to these rules, and one draw needn't show every extreme that they name: With p = s for every slab s, or p = 63 - s for every slab s, and one whole number c of 1 to 32: slab_rank is p where p >= c and p - 64 where p < c.
All inputs are finite; a program needn't handle non-finite values.
Results may differ from the reference program's by a relative error of at most 0.00079.
Values may be sent and summed in bfloat16 or wider, within the bound.
No kernel may reach another device: no remote copies, remote signals or barrier semaphores. Data moves between devices by JAX's collectives and lax.ppermute only.
A program may use at most 192 MiB of HBM per device.

```python
import jax
import jax.numpy as jnp
from jax import lax

DEP = 4
BRICK = 4
NZ = 256
ROWS = 512
COLS = 512


def draw_slab_rank(key, part):
    slabs = NZ // DEP
    flag = jax.random.randint(jax.random.fold_in(key, 17), (), 0, 2)
    offset = jax.random.randint(jax.random.fold_in(key, 29), (), 1, slabs // 2 + 1)
    counted = jnp.arange(slabs, dtype=jnp.int32)
    position = jnp.where(flag == 1, counted, slabs - 1 - counted)
    ranks = jnp.where(position >= offset, position, position - slabs)
    return ranks.astype(jnp.int32)


def touch_ends(drawn, key, least, top_value):
    extent = drawn.shape
    place = [jax.random.randint(jax.random.fold_in(key, axis), (), 0, extent[axis]) for axis in range(len(extent))]
    drawn = drawn.at[tuple(place)].set(least)
    longest = extent.index(max(extent))
    place[longest] = (place[longest] + 1) % extent[longest]
    return drawn.at[tuple(place)].set(top_value)


def block_levels(stream_key, extent, shards, low, high):
    level, own = 1.0, jax.random.fold_in(stream_key, 6)
    for dim, parts in shards:
        steps = jnp.exp(jax.random.uniform(jax.random.fold_in(own, dim), (parts,), jnp.float32, low / len(shards), high / len(shards)))
        level = level * jnp.repeat(steps, extent[dim] // parts).reshape([-1 if axis == dim else 1 for axis in range(len(extent))])
    return level


def centred(stream_key, shape, deviation, most, cuts=(), kind=jnp.bfloat16):
    result = deviation * jax.random.normal(stream_key, shape, jnp.float32)
    if cuts:
        result = result * block_levels(stream_key, shape, cuts, -0.22, 0.18)
    return jnp.clip(result, -most, most).astype(kind)


def setup_inputs(seed: int = 0) -> dict:
    key_list = jax.random.split(jax.random.key(seed), 8)
    coarse = centred(key_list[0], (NZ // 2, ROWS // 2, COLS // 2), 1.0, 6.0, ((0, 64), (2, 4)))
    residual = centred(key_list[1], (NZ, ROWS, COLS), 1.0, 6.0, ((0, 64), (2, 4)))
    levels = touch_ends(jax.random.randint(key_list[2], (NZ // BRICK, ROWS // BRICK, COLS // BRICK), 0, 3), jax.random.fold_in(key_list[2], 1), 0, 2).astype(jnp.int32)
    slab_rank = draw_slab_rank(jax.random.fold_in(key_list[7], 71), 0)
    light_angles = jnp.clip(jax.random.uniform(key_list[4], (2,), jnp.float32, -3.140625, 3.140625), -3.140625, 3.140625)
    color_slope = jnp.clip(jax.random.uniform(key_list[5], (3,), jnp.float32, 0.5, 2.0), 0.5, 2.0)
    color_shift = jnp.clip(jax.random.uniform(key_list[6], (3,), jnp.float32, -1.0, 1.0), -1.0, 1.0)
    return dict(coarse=coarse, residual=residual, levels=levels, slab_rank=slab_rank, light_angles=light_angles, color_slope=color_slope, color_shift=color_shift)


def refine_block(coarse_part, residual_part, level_part):
    dep, rows, cols = residual_part.shape
    lifted = coarse_part.astype(jnp.float32)[:, None, :, None, :, None]
    lifted = jnp.broadcast_to(lifted, (dep // 2, 2, rows // 2, 2, cols // 2, 2)).reshape(dep, rows, cols)
    nb = level_part.shape
    scaled = level_part.astype(jnp.float32)[:, None, :, None, :, None]
    scaled = jnp.broadcast_to(scaled, (nb[0], dep // nb[0], nb[1], rows // nb[1], nb[2], cols // nb[2])).reshape(dep, rows, cols)
    return (lifted + 0.5 * scaled * residual_part.astype(jnp.float32)).astype(jnp.bfloat16)

def light_vector(angles):
    return jnp.stack([jnp.sin(angles[1]), jnp.cos(angles[1]) * jnp.sin(angles[0]), jnp.cos(angles[1]) * jnp.cos(angles[0])])

def render_slab(padded, ascending, step, light, slope, shift):
    f = padded.astype(jnp.float32)
    v = f[2:-2, 2:-2, 2:-2]
    grad_z = (f[:-4, 2:-2, 2:-2] - 8.0 * f[1:-3, 2:-2, 2:-2] + 8.0 * f[3:-1, 2:-2, 2:-2] - f[4:, 2:-2, 2:-2]) / 12.0
    grad_y = (f[2:-2, :-4, 2:-2] - 8.0 * f[2:-2, 1:-3, 2:-2] + 8.0 * f[2:-2, 3:-1, 2:-2] - f[2:-2, 4:, 2:-2]) / 12.0
    grad_x = (f[2:-2, 2:-2, :-4] - 8.0 * f[2:-2, 2:-2, 1:-3] + 8.0 * f[2:-2, 2:-2, 3:-1] - f[2:-2, 2:-2, 4:]) / 12.0
    along = light[0] * grad_z + light[1] * grad_y + light[2] * grad_x
    shade = 0.25 + 0.75 * jnp.abs(along) / jnp.sqrt(grad_z * grad_z + grad_y * grad_y + grad_x * grad_x + 1.0)
    extinct = 4.0 * jax.nn.sigmoid(3.0 * (v - 1.5))
    running = jnp.cumsum(extinct, axis=0)
    total = running[-1]
    before = jnp.where(ascending, running - extinct, total - running)
    weight = jnp.exp(-step * before) * (1.0 - jnp.exp(-step * extinct)) * shade
    colors = [lax.optimization_barrier(jnp.sum(weight * jax.nn.sigmoid(slope[k] * v + shift[k]), axis=0)) for k in range(3)]
    return (jnp.stack(colors + [1.0 - jnp.exp(-step * total)]), lax.optimization_barrier(jnp.mean(shade, axis=0)))

def reference(coarse, residual, levels, slab_rank, light_angles, color_slope, color_shift):
    slabs = NZ // DEP

    def refine(s):
        c = lax.dynamic_slice_in_dim(coarse, s * (DEP // 2), DEP // 2, 0)
        r = lax.dynamic_slice_in_dim(residual, s * DEP, DEP, 0)
        l = lax.dynamic_slice_in_dim(levels, s * (DEP // BRICK), DEP // BRICK, 0)
        return refine_block(c, r, l)
    refined = lax.map(refine, jnp.arange(slabs, dtype=jnp.int32)).reshape(NZ, ROWS, COLS)
    padded = jnp.pad(refined, 2)
    ascending = slab_rank[0] < slab_rank[slabs - 1]
    order = jnp.argsort(slab_rank).astype(jnp.int32)
    light = light_vector(light_angles)
    step = 4.0 / NZ

    def composite(carry, k):
        total, through = carry
        s = order[k]
        piece = lax.dynamic_slice_in_dim(padded, (s * DEP).astype(jnp.int32), DEP + 4, 0)
        slab_image, mean_shade = render_slab(piece, ascending, step, light, color_slope, color_shift)
        visible = (slab_rank[s] >= 0).astype(jnp.float32)
        slab_image = slab_image * visible
        total = total + through[None] * slab_image
        through = through * (1.0 - slab_image[3])
        return ((total, through), mean_shade)
    start = (jnp.zeros((4, ROWS, COLS), jnp.float32), jnp.ones((ROWS, COLS), jnp.float32))
    (image, _), shades = lax.scan(composite, start, jnp.arange(slabs, dtype=jnp.int32))
    slab_shade = jnp.zeros((slabs, ROWS, COLS), jnp.float32).at[order].set(shades)
    return (image, slab_shade)
```

```python
import jax
import jax.numpy as jnp
from jax import lax
from jax.experimental import pallas as pl
from jax.experimental.pallas import tpu as pltpu
from jax.sharding import PartitionSpec as P

F32 = jnp.float32
BF16 = jnp.bfloat16
VMEM = pl.BlockSpec(memory_space=pltpu.VMEM)
SMEM = pl.BlockSpec(memory_space=pltpu.SMEM)
NN = (((1,), (0,)), ((), ()))
NT = (((1,), (1,)), ((), ()))
PAD = 64
BLK = 128
SUB = 16


def dot(a, b, dims=NN):
    return lax.dot_general(a, b, dims, preferred_element_type=F32)


def iota2(shape):
    return (
        lax.broadcasted_iota(jnp.int32, shape, 0),
        lax.broadcasted_iota(jnp.int32, shape, 1),
    )


def repeater(out, inner):
    r, c = iota2((out, inner))
    return jnp.where(r // (out // inner) == c, 1.0, 0.0).astype(BF16)


def stencil(offset):
    w = jnp.where(offset == -2, 1.0, jnp.where(offset == -1, -8.0, 0.0))
    return jnp.where(offset == 1, 8.0, jnp.where(offset == 2, -1.0, w))


def refine_kernel(res_ref, coarse_ref, level_ref, low_ref, high_ref, up_ref, down_ref):
    dep, rows, cols = res_ref.shape
    half = coarse_ref.shape[2]
    widen2 = repeater(cols, coarse_ref.shape[1])
    widen4 = repeater(cols, level_ref.shape[0])
    lev = dot(widen4, level_ref[...].astype(F32).astype(BF16)).astype(BF16)
    scale = 0.5 * dot(repeater(rows, lev.shape[1]), lev, NT)
    tall2 = repeater(256, 128)
    k, c = iota2((16, cols))
    edges = jnp.zeros((16, rows), F32)
    for zc in range(dep // 2):
        wide = dot(widen2, coarse_ref[zc]).astype(BF16)
        lifted = [dot(tall2, wide[:, b * 128 : (b + 1) * 128], NT) for b in range(half // 128)]
        for z in (2 * zc, 2 * zc + 1):
            out = low_ref if z < 2 else high_ref
            for b in range(half // 128):
                part = pl.ds(b * 256, 256)
                out[z % 2, part, :] = (
                    lifted[b] + scale[b * 256 : (b + 1) * 256] * res_ref[z, part, :].astype(F32)
                ).astype(BF16)
            col = jnp.where(k < 8, k - 2 * z + cols - 2, k - 8 - 2 * z)
            mine = (k % 8) // 2 == z
            pick = jnp.where(mine & (col == c), 1.0, 0.0).astype(BF16)
            edges = edges + dot(pick, out[z % 2], NT)
    up_ref[...] = edges[0:8].astype(BF16)
    down_ref[...] = edges[8:16].astype(BF16)


def refine(residual, coarse, levels):
    dep, rows, cols = residual.shape
    plane = jax.ShapeDtypeStruct((dep // 2, rows, cols), BF16)
    edge = jax.ShapeDtypeStruct((2 * dep, rows), BF16)
    return pl.pallas_call(
        refine_kernel,
        out_shape=(plane, plane, edge, edge),
        in_specs=[VMEM] * 3,
        out_specs=(VMEM,) * 4,
        name="refine",
    )(residual, jnp.swapaxes(coarse, 1, 2), jnp.swapaxes(levels[0], 0, 1))


def render_kernel(
    step, low_ref, high_ref, before_ref, after_ref, left_ref, right_ref,
    rank_ref, angle_ref, slope_ref, shift_ref, image_ref, shade_ref, pair, gx_ref, gy_ref,
):
    _, rows, cols = low_ref.shape
    slabs = rank_ref.shape[0]
    ascending = rank_ref[0] < rank_ref[slabs - 1]
    visible = jnp.where(rank_ref[lax.axis_index("depth")] >= 0, 1.0, 0.0).astype(F32)
    azimuth = jnp.full((SUB, cols), angle_ref[0], F32)
    elevation = jnp.full((SUB, cols), angle_ref[1], F32)
    light_z = jnp.sin(elevation)
    light_y = jnp.cos(elevation) * jnp.sin(azimuth)
    light_x = jnp.cos(elevation) * jnp.cos(azimuth)
    slope = [0.5 * slope_ref[k] for k in range(3)]
    shift = [0.5 * shift_ref[k] for k in range(3)]

    zero = jnp.zeros((PAD, 2 * cols), BF16)
    for p, ref in enumerate((low_ref, high_ref)):
        pair[p, 0:PAD, :] = zero
        pair[p, PAD + rows :, :] = zero
        for q in range(2):
            pair[p, PAD : PAD + rows, q * cols : (q + 1) * cols] = ref[q]

    r, c = iota2((cols, cols))
    across = stencil(r - c).astype(BF16)
    r, c = iota2((BLK, BLK + 2 * PAD))
    along = stencil(c - PAD - r).astype(BF16)
    k, c = iota2((16, cols))
    spot = jnp.where(k < 8, k % 2 - 2, cols + k % 2)
    beside = [
        jnp.where((k % 8) // 2 == z, stencil(spot - c), 0.0).astype(BF16) for z in range(4)
    ]
    columns = jnp.concatenate([left_ref[...].astype(F32), right_ref[...].astype(F32)], 0)
    columns = columns.T.astype(BF16)

    for b in range(rows // BLK):
        base = b * BLK
        for p, ref in enumerate((low_ref, high_ref)):
            gy_ref[p] = dot(along, pair[p, base : base + BLK + 2 * PAD, :])
            for q in range(2):
                gx_ref[2 * p + q] = dot(ref[q, base : base + BLK, :], across) + dot(
                    columns[base : base + BLK], beside[2 * p + q]
                )

        def shade_rows(i, carry, base=base):
            at = pl.ds(pl.multiple_of(i * SUB, SUB), SUB)
            row = pl.ds(pl.multiple_of(base + i * SUB, SUB), SUB)
            planes = [
                ref[q, row, :].astype(F32)
                for ref in (before_ref, low_ref, high_ref, after_ref)
                for q in range(2)
            ]
            clear, alpha, shade, color = [], [], [], []
            for z in range(4):
                v = planes[z + 2]
                gz = (planes[z] - planes[z + 4]) + 8.0 * (planes[z + 3] - planes[z + 1])
                gy = gy_ref[z // 2, at, (z % 2) * cols : (z % 2 + 1) * cols]
                gx = gx_ref[z, at, :]
                lit = light_z * gz + light_y * gy + light_x * gx
                size = gz * gz + gy * gy + gx * gx + 144.0
                shade.append(0.25 + 0.75 * (jnp.abs(lit) * lax.rsqrt(size)))
                extinct = 2.0 + 2.0 * jnp.tanh(1.5 * v - 2.25)
                clear.append(jnp.exp(-step * extinct))
                alpha.append((1.0 - clear[z]) * shade[z])
                color.append([0.5 + 0.5 * jnp.tanh(slope[n] * v + shift[n]) for n in range(3)])
            up = [None, clear[0], clear[0] * clear[1], None]
            up[3] = up[2] * clear[2]
            down = [None, None, clear[3], None]
            down[1] = clear[3] * clear[2]
            down[0] = down[1] * clear[1]
            before = [
                jnp.where(ascending, 1.0, down[0]),
                jnp.where(ascending, up[1], down[1]),
                jnp.where(ascending, up[2], down[2]),
                jnp.where(ascending, up[3], 1.0),
            ]
            weight = [before[z] * alpha[z] * visible for z in range(4)]
            out = [
                (weight[0] * color[0][n] + weight[1] * color[1][n])
                + (weight[2] * color[2][n] + weight[3] * color[3][n])
                for n in range(3)
            ]
            out.append((1.0 - up[3] * clear[3]) * visible)
            for half in range(SUB // 8):
                tile = jnp.concatenate([x[half * 8 : half * 8 + 8] for x in out], 0)
                image_ref[(base // 8) + i * (SUB // 8) + half] = tile.astype(image_ref.dtype)
            shade_ref[0, row, :] = 0.25 * ((shade[0] + shade[1]) + (shade[2] + shade[3]))
            return carry

        lax.fori_loop(0, BLK // SUB, shade_rows, 0, unroll=2)


def render(step, low, high, before, after, left, right, rank, angles, slope, shift):
    _, rows, cols = low.shape
    return pl.pallas_call(
        lambda *refs: render_kernel(step, *refs),
        out_shape=(
            jax.ShapeDtypeStruct((rows // 8, 32, cols), BF16),
            jax.ShapeDtypeStruct((1, rows, cols), F32),
        ),
        in_specs=[VMEM] * 6 + [SMEM] * 4,
        out_specs=(VMEM, VMEM),
        scratch_shapes=[
            pltpu.VMEM((2, rows + 2 * PAD, 2 * cols), BF16),
            pltpu.VMEM((4, BLK, cols), F32),
            pltpu.VMEM((2, BLK, 2 * cols), F32),
        ],
        name="render",
    )(low, high, before, after, left, right, rank, angles, slope, shift)


def compose_kernel(part_ref, rank_ref, image_ref):
    slabs = part_ref.shape[0]
    cols = part_ref.shape[2]
    ascending = rank_ref[0] < rank_ref[slabs - 1]

    def body(i, carry):
        through, red, green, blue = carry
        tile = part_ref[jnp.where(ascending, i, slabs - 1 - i)].astype(F32)
        red = red + through * tile[0:8]
        green = green + through * tile[8:16]
        blue = blue + through * tile[16:24]
        return (through * (1.0 - tile[24:32]), red, green, blue)

    zero = jnp.zeros((8, cols), F32)
    through, red, green, blue = lax.fori_loop(
        0, slabs, body, (jnp.ones((8, cols), F32), zero, zero, zero), unroll=8
    )
    image_ref[0] = red
    image_ref[1] = green
    image_ref[2] = blue
    image_ref[3] = 1.0 - through


def compose(parts, rank):
    return pl.pallas_call(
        compose_kernel,
        out_shape=jax.ShapeDtypeStruct((4, 8, parts.shape[2]), F32),
        in_specs=[VMEM, SMEM],
        out_specs=VMEM,
        name="compose",
    )(parts, rank)


def shards(coarse, residual, levels, slab_rank, light_angles, color_slope, color_shift):
    dep = residual.shape[0]
    slabs, tiles = lax.axis_size("depth"), lax.axis_size("tile")
    step = 4.0 / (dep * slabs)
    low, high, up, down = refine(residual, coarse, levels)
    fore = lambda n: [(i, i + 1) for i in range(n - 1)]
    back = lambda n: [(i + 1, i) for i in range(n - 1)]
    before = lax.ppermute(high, "depth", fore(slabs))
    after = lax.ppermute(low, "depth", back(slabs))
    left = lax.ppermute(up, "tile", fore(tiles))
    right = lax.ppermute(down, "tile", back(tiles))
    image, shade = render(
        step, low, high, before, after, left, right,
        slab_rank, light_angles, color_slope, color_shift,
    )
    parts = lax.all_to_all(image, "depth", split_axis=0, concat_axis=0, tiled=True)
    return (compose(parts, slab_rank), shade)


def solution(mesh):
    placed = (
        P("depth", None, "tile"),
        P("depth", None, "tile"),
        P("depth", None, "tile"),
        P(),
        P(),
        P(),
        P(),
    )
    return jax.shard_map(
        shards,
        mesh=mesh,
        in_specs=placed,
        out_specs=(P(None, "depth", "tile"), P("depth", None, "tile")),
        check_vma=False,
    )
```

```python
import jax
import jax.numpy as jnp
from jax import lax
from jax.experimental import pallas as pl
from jax.experimental.pallas import tpu as pltpu
from jax.sharding import PartitionSpec as P

F32 = jnp.float32
BF16 = jnp.bfloat16
VMEM = pl.BlockSpec(memory_space=pltpu.VMEM)
SMEM = pl.BlockSpec(memory_space=pltpu.SMEM)
NN = (((1,), (0,)), ((), ()))
NT = (((1,), (1,)), ((), ()))
PAD = 64
BLK = 128
SUB = 16


def near(x):
    return pltpu.with_memory_space_constraint(x, pltpu.VMEM)


def dot(a, b, dims=NN):
    return lax.dot_general(a, b, dims, preferred_element_type=F32)


def iota2(shape):
    return (
        lax.broadcasted_iota(jnp.int32, shape, 0),
        lax.broadcasted_iota(jnp.int32, shape, 1),
    )


def repeater(out, inner):
    r, c = iota2((out, inner))
    return jnp.where(r // (out // inner) == c, 1.0, 0.0).astype(BF16)


def stencil(offset):
    w = jnp.where(offset == -2, 1.0, jnp.where(offset == -1, -8.0, 0.0))
    return jnp.where(offset == 1, 8.0, jnp.where(offset == 2, -1.0, w))


def refine_kernel(res_ref, coarse_ref, level_ref, low_ref, high_ref, up_ref, down_ref):
    dep, rows, cols = res_ref.shape
    half = coarse_ref.shape[2]
    widen2 = repeater(cols, coarse_ref.shape[1])
    widen4 = repeater(cols, level_ref.shape[0])
    lev = dot(widen4, level_ref[...].astype(F32).astype(BF16)).astype(BF16)
    scale = 0.5 * dot(repeater(rows, lev.shape[1]), lev, NT)
    tall2 = repeater(256, 128)
    k, c = iota2((16, cols))
    edges = jnp.zeros((16, rows), F32)
    for zc in range(dep // 2):
        wide = dot(widen2, coarse_ref[zc]).astype(BF16)
        lifted = [dot(tall2, wide[:, b * 128 : (b + 1) * 128], NT) for b in range(half // 128)]
        for z in (2 * zc, 2 * zc + 1):
            out = low_ref if z < 2 else high_ref
            for b in range(half // 128):
                part = pl.ds(b * 256, 256)
                out[z % 2, part, :] = (
                    lifted[b] + scale[b * 256 : (b + 1) * 256] * res_ref[z, part, :].astype(F32)
                ).astype(BF16)
            col = jnp.where(k < 8, k - 2 * z + cols - 2, k - 8 - 2 * z)
            mine = (k % 8) // 2 == z
            pick = jnp.where(mine & (col == c), 1.0, 0.0).astype(BF16)
            edges = edges + dot(pick, out[z % 2], NT)
    up_ref[...] = edges[0:8].astype(BF16)
    down_ref[...] = edges[8:16].astype(BF16)


def refine(residual, coarse, levels):
    dep, rows, cols = residual.shape
    plane = pltpu.VMEM((dep // 2, rows, cols), BF16)
    edge = pltpu.VMEM((2 * dep, rows), BF16)
    return pl.pallas_call(
        refine_kernel,
        out_shape=(plane, plane, edge, edge),
        in_specs=[VMEM] * 3,
        out_specs=(VMEM,) * 4,
        name="refine",
    )(residual, jnp.swapaxes(coarse, 1, 2), jnp.swapaxes(levels[0], 0, 1))


def render_kernel(
    step, low_ref, high_ref, before_ref, after_ref, left_ref, right_ref,
    rank_ref, angle_ref, slope_ref, shift_ref, image_ref, shade_ref, pair, gx_ref, gy_ref,
):
    _, rows, cols = low_ref.shape
    slabs = rank_ref.shape[0]
    ascending = rank_ref[0] < rank_ref[slabs - 1]
    visible = jnp.where(rank_ref[lax.axis_index("depth")] >= 0, 1.0, 0.0).astype(F32)
    azimuth = jnp.full((SUB, cols), angle_ref[0], F32)
    elevation = jnp.full((SUB, cols), angle_ref[1], F32)
    light_z = jnp.sin(elevation)
    light_y = jnp.cos(elevation) * jnp.sin(azimuth)
    light_x = jnp.cos(elevation) * jnp.cos(azimuth)
    slope = [0.5 * slope_ref[k] for k in range(3)]
    shift = [0.5 * shift_ref[k] for k in range(3)]

    zero = jnp.zeros((PAD, 2 * cols), BF16)
    for p, ref in enumerate((low_ref, high_ref)):
        pair[p, 0:PAD, :] = zero
        pair[p, PAD + rows :, :] = zero
        for q in range(2):
            pair[p, PAD : PAD + rows, q * cols : (q + 1) * cols] = ref[q]

    r, c = iota2((cols, cols))
    across = stencil(r - c).astype(BF16)
    r, c = iota2((BLK, BLK + 2 * PAD))
    along = stencil(c - PAD - r).astype(BF16)
    k, c = iota2((16, cols))
    spot = jnp.where(k < 8, k % 2 - 2, cols + k % 2)
    beside = [
        jnp.where((k % 8) // 2 == z, stencil(spot - c), 0.0).astype(BF16) for z in range(4)
    ]
    columns = jnp.concatenate([left_ref[...].astype(F32), right_ref[...].astype(F32)], 0)
    columns = columns.T.astype(BF16)

    for b in range(rows // BLK):
        base = b * BLK
        for p, ref in enumerate((low_ref, high_ref)):
            gy_ref[p] = dot(along, pair[p, base : base + BLK + 2 * PAD, :])
            for q in range(2):
                gx_ref[2 * p + q] = dot(ref[q, base : base + BLK, :], across) + dot(
                    columns[base : base + BLK], beside[2 * p + q]
                )

        def shade_rows(i, carry, base=base):
            at = pl.ds(pl.multiple_of(i * SUB, SUB), SUB)
            row = pl.ds(pl.multiple_of(base + i * SUB, SUB), SUB)
            planes = [
                ref[q, row, :].astype(F32)
                for ref in (before_ref, low_ref, high_ref, after_ref)
                for q in range(2)
            ]
            clear, alpha, shade, color = [], [], [], []
            for z in range(4):
                v = planes[z + 2]
                gz = (planes[z] - planes[z + 4]) + 8.0 * (planes[z + 3] - planes[z + 1])
                gy = gy_ref[z // 2, at, (z % 2) * cols : (z % 2 + 1) * cols]
                gx = gx_ref[z, at, :]
                lit = light_z * gz + light_y * gy + light_x * gx
                size = gz * gz + gy * gy + gx * gx + 144.0
                shade.append(0.25 + 0.75 * (jnp.abs(lit) * lax.rsqrt(size)))
                extinct = 2.0 + 2.0 * jnp.tanh(1.5 * v - 2.25)
                clear.append(jnp.exp(-step * extinct))
                alpha.append((1.0 - clear[z]) * shade[z])
                color.append([0.5 + 0.5 * jnp.tanh(slope[n] * v + shift[n]) for n in range(3)])
            up = [None, clear[0], clear[0] * clear[1], None]
            up[3] = up[2] * clear[2]
            down = [None, None, clear[3], None]
            down[1] = clear[3] * clear[2]
            down[0] = down[1] * clear[1]
            before = [
                jnp.where(ascending, 1.0, down[0]),
                jnp.where(ascending, up[1], down[1]),
                jnp.where(ascending, up[2], down[2]),
                jnp.where(ascending, up[3], 1.0),
            ]
            weight = [before[z] * alpha[z] * visible for z in range(4)]
            out = [
                (weight[0] * color[0][n] + weight[1] * color[1][n])
                + (weight[2] * color[2][n] + weight[3] * color[3][n])
                for n in range(3)
            ]
            out.append((1.0 - up[3] * clear[3]) * visible)
            for half in range(SUB // 8):
                tile = jnp.concatenate([x[half * 8 : half * 8 + 8] for x in out], 0)
                image_ref[(base // 8) + i * (SUB // 8) + half] = tile.astype(image_ref.dtype)
            shade_ref[0, row, :] = 0.25 * ((shade[0] + shade[1]) + (shade[2] + shade[3]))
            return carry

        lax.fori_loop(0, BLK // SUB, shade_rows, 0, unroll=2)


def render(step, low, high, before, after, left, right, rank, angles, slope, shift):
    _, rows, cols = low.shape
    return pl.pallas_call(
        lambda *refs: render_kernel(step, *refs),
        out_shape=(
            pltpu.VMEM((rows // 8, 32, cols), BF16),
            jax.ShapeDtypeStruct((1, rows, cols), F32),
        ),
        in_specs=[VMEM] * 6 + [SMEM] * 4,
        out_specs=(VMEM, VMEM),
        scratch_shapes=[
            pltpu.VMEM((2, rows + 2 * PAD, 2 * cols), BF16),
            pltpu.VMEM((4, BLK, cols), F32),
            pltpu.VMEM((2, BLK, 2 * cols), F32),
        ],
        name="render",
    )(*(near(x) for x in (low, high, before, after, left, right)), rank, angles, slope, shift)


def compose_kernel(part_ref, rank_ref, image_ref):
    slabs = part_ref.shape[0]
    cols = part_ref.shape[2]
    ascending = rank_ref[0] < rank_ref[slabs - 1]

    def body(i, carry):
        through, red, green, blue = carry
        tile = part_ref[jnp.where(ascending, i, slabs - 1 - i)].astype(F32)
        red = red + through * tile[0:8]
        green = green + through * tile[8:16]
        blue = blue + through * tile[16:24]
        return (through * (1.0 - tile[24:32]), red, green, blue)

    zero = jnp.zeros((8, cols), F32)
    through, red, green, blue = lax.fori_loop(
        0, slabs, body, (jnp.ones((8, cols), F32), zero, zero, zero), unroll=8
    )
    image_ref[0] = red
    image_ref[1] = green
    image_ref[2] = blue
    image_ref[3] = 1.0 - through


def compose(parts, rank):
    return pl.pallas_call(
        compose_kernel,
        out_shape=jax.ShapeDtypeStruct((4, 8, parts.shape[2]), F32),
        in_specs=[VMEM, SMEM],
        out_specs=VMEM,
        name="compose",
    )(near(parts), rank)


def shards(coarse, residual, levels, slab_rank, light_angles, color_slope, color_shift):
    dep = residual.shape[0]
    slabs, tiles = lax.axis_size("depth"), lax.axis_size("tile")
    step = 4.0 / (dep * slabs)
    low, high, up, down = refine(residual, coarse, levels)
    fore = lambda n: [(i, i + 1) for i in range(n - 1)]
    back = lambda n: [(i + 1, i) for i in range(n - 1)]
    before = lax.ppermute(high, "depth", fore(slabs))
    after = lax.ppermute(low, "depth", back(slabs))
    left = lax.ppermute(up, "tile", fore(tiles))
    right = lax.ppermute(down, "tile", back(tiles))
    image, shade = render(
        step, low, high, before, after, left, right,
        slab_rank, light_angles, color_slope, color_shift,
    )
    parts = lax.all_to_all(image, "depth", split_axis=0, concat_axis=0, tiled=True)
    return (compose(parts, slab_rank), shade)


def solution(mesh):
    placed = (
        P("depth", None, "tile"),
        P("depth", None, "tile"),
        P("depth", None, "tile"),
        P(),
        P(),
        P(),
        P(),
    )
    return jax.shard_map(
        shards,
        mesh=mesh,
        in_specs=placed,
        out_specs=(P(None, "depth", "tile"), P("depth", None, "tile")),
        check_vma=False,
    )
```

```python
import jax
import jax.numpy as jnp
from jax import lax
from jax.experimental import pallas as pl
from jax.experimental.pallas import tpu as pltpu
from jax.sharding import PartitionSpec as P

F32 = jnp.float32
BF16 = jnp.bfloat16
VMEM = pl.BlockSpec(memory_space=pltpu.VMEM)
SMEM = pl.BlockSpec(memory_space=pltpu.SMEM)
NN = (((1,), (0,)), ((), ()))
NT = (((1,), (1,)), ((), ()))
PAD = 64
BLK = 128
SUB = 16


GRANT = pltpu.CompilerParams(vmem_limit_bytes=12 * 2**20)
GAIN = 16.0


def far(x):
    return pltpu.with_memory_space_constraint(x, pltpu.HBM)


def near(x):
    return pltpu.with_memory_space_constraint(x, pltpu.VMEM)


def dot(a, b, dims=NN):
    return lax.dot_general(a, b, dims, preferred_element_type=F32)


def iota2(shape):
    return (
        lax.broadcasted_iota(jnp.int32, shape, 0),
        lax.broadcasted_iota(jnp.int32, shape, 1),
    )


def repeater(out, inner):
    r, c = iota2((out, inner))
    return jnp.where(r // (out // inner) == c, 1.0, 0.0).astype(BF16)


def stencil(offset):
    w = jnp.where(offset == -2, 1.0, jnp.where(offset == -1, -8.0, 0.0))
    return jnp.where(offset == 1, 8.0, jnp.where(offset == 2, -1.0, w))


def encode(x):
    x = x * GAIN
    x = x * x
    return x * x


def decode(x):
    for _ in range(2):
        x = x * lax.rsqrt(jnp.maximum(x, 1e-37))
    return x * (1.0 / GAIN)


def refine_kernel(
    res_ref, coarse_ref, level_ref, full_ref, z1_ref, z2_ref, x1_ref, x2_ref
):
    dep, rows, cols = res_ref.shape
    half = coarse_ref.shape[2]
    even_z = lax.rem(lax.axis_index("depth"), 2) == 0
    even_x = lax.rem(lax.axis_index("tile"), 2) == 0
    widen2 = repeater(cols, coarse_ref.shape[1])
    widen4 = repeater(cols, level_ref.shape[0])
    lev = dot(widen4, level_ref[...].astype(F32).astype(BF16)).astype(BF16)
    scale = 0.5 * dot(repeater(rows, lev.shape[1]), lev, NT)
    tall2 = repeater(256, 128)
    k, c = iota2((16, cols))
    edges = jnp.zeros((16, rows), F32)
    for zc in range(dep // 2):
        wide = dot(widen2, coarse_ref[zc]).astype(BF16)
        lifted = [dot(tall2, wide[:, b * 128 : (b + 1) * 128], NT) for b in range(half // 128)]
        for z in (2 * zc, 2 * zc + 1):
            for b in range(half // 128):
                part = pl.ds(b * 256, 256)
                full_ref[z, part, :] = (
                    lifted[b] + scale[b * 256 : (b + 1) * 256] * res_ref[z, part, :].astype(F32)
                ).astype(BF16)
            col = jnp.where(k < 8, k - 2 * z + cols - 2, k - 8 - 2 * z)
            mine = (k % 8) // 2 == z
            pick = jnp.where(mine & (col == c), 1.0, 0.0).astype(BF16)
            edges = edges + dot(pick, full_ref[z], NT)
    for p in range(2):
        z1_ref[p] = jnp.where(even_z, full_ref[2 + p], full_ref[p])
        z2_ref[p] = jnp.where(even_z, full_ref[p], full_ref[2 + p])
    last, first = edges[0:8], edges[8:16]
    x1_ref[...] = jnp.where(even_x, last, first).astype(BF16)
    x2_ref[...] = jnp.where(even_x, first, last).astype(BF16)


def refine(residual, coarse, levels):
    dep, rows, cols = residual.shape
    plane = pltpu.VMEM((2, rows, cols), BF16)
    edge = pltpu.VMEM((2 * dep, rows), BF16)
    return pl.pallas_call(
        refine_kernel,
        out_shape=(pltpu.VMEM((dep, rows, cols), BF16), plane, plane, edge, edge),
        in_specs=[VMEM] * 3,
        out_specs=(VMEM,) * 5,
        cost_estimate=pl.CostEstimate(flops=10**8, bytes_accessed=10**6, transcendentals=0),
        compiler_params=GRANT,
        name="refine",
    )(*(far(x) for x in (residual, jnp.swapaxes(coarse, 1, 2), jnp.swapaxes(levels[0], 0, 1))))


def prepare_kernel(
    step, full_ref, x1_ref, x2_ref, rank_ref, angle_ref, slope_ref, shift_ref,
    lit_ref, size_ref, coef_ref, cover_ref, flag_ref, pair, gx_ref, gy_ref,
):
    dep, rows, cols = full_ref.shape
    slabs = rank_ref.shape[0]
    even_x = lax.rem(lax.axis_index("tile"), 2) == 0
    ascending = rank_ref[0] < rank_ref[slabs - 1]
    visible = jnp.where(rank_ref[lax.axis_index("depth")] >= 0, 1.0, 0.0).astype(F32)
    azimuth = jnp.full((SUB, cols), angle_ref[0], F32)
    elevation = jnp.full((SUB, cols), angle_ref[1], F32)
    light_y = jnp.cos(elevation) * jnp.sin(azimuth)
    light_x = jnp.cos(elevation) * jnp.cos(azimuth)
    slope = [0.5 * slope_ref[k] for k in range(3)]
    shift = [0.5 * shift_ref[k] for k in range(3)]
    flag_ref[0] = jnp.sin(elevation)
    flag_ref[1] = jnp.full((SUB, cols), jnp.where(ascending, 1.0, 0.0), F32)

    zero = jnp.zeros((PAD, 2 * cols), BF16)
    for p in range(2):
        pair[p, 0:PAD, :] = zero
        pair[p, PAD + rows :, :] = zero
        for q in range(2):
            pair[p, PAD : PAD + rows, q * cols : (q + 1) * cols] = full_ref[2 * p + q]

    r, c = iota2((cols, cols))
    across = stencil(r - c).astype(BF16)
    r, c = iota2((BLK, BLK + 2 * PAD))
    along = stencil(c - PAD - r).astype(BF16)
    k, c = iota2((16, cols))
    spot = jnp.where(k < 8, k % 2 - 2, cols + k % 2)
    beside = [
        jnp.where((k % 8) // 2 == z, stencil(spot - c), 0.0).astype(BF16) for z in range(4)
    ]
    x1, x2 = x1_ref[...].astype(F32), x2_ref[...].astype(F32)
    columns = jnp.concatenate([jnp.where(even_x, x2, x1), jnp.where(even_x, x1, x2)], 0)
    columns = columns.T.astype(BF16)

    for b in range(rows // BLK):
        base = b * BLK
        for p in range(2):
            gy_ref[p] = dot(along, pair[p, base : base + BLK + 2 * PAD, :])
            for q in range(2):
                z = 2 * p + q
                gx_ref[z] = dot(full_ref[z, base : base + BLK, :], across) + dot(
                    columns[base : base + BLK], beside[z]
                )

        def some_rows(i, carry, base=base):
            at = pl.ds(pl.multiple_of(i * SUB, SUB), SUB)
            row = pl.ds(pl.multiple_of(base + i * SUB, SUB), SUB)
            clear, color = [], []
            for z in range(4):
                v = full_ref[z, row, :].astype(F32)
                gy = gy_ref[z // 2, at, (z % 2) * cols : (z % 2 + 1) * cols]
                gx = gx_ref[z, at, :]
                lit_ref[z, row, :] = light_y * gy + light_x * gx
                size_ref[z, row, :] = gy * gy + gx * gx + 144.0
                extinct = 2.0 + 2.0 * jnp.tanh(1.5 * v - 2.25)
                clear.append(jnp.exp(-step * extinct))
                color.append([0.5 + 0.5 * jnp.tanh(slope[n] * v + shift[n]) for n in range(3)])
            up = [None, clear[0], clear[0] * clear[1], None]
            up[3] = up[2] * clear[2]
            down = [None, None, clear[3], None]
            down[1] = clear[3] * clear[2]
            down[0] = down[1] * clear[1]
            before = [
                jnp.where(ascending, 1.0, down[0]),
                jnp.where(ascending, up[1], down[1]),
                jnp.where(ascending, up[2], down[2]),
                jnp.where(ascending, up[3], 1.0),
            ]
            for z in range(4):
                weight = before[z] * (1.0 - clear[z]) * visible
                for n in range(3):
                    coef_ref[3 * z + n, row, :] = weight * color[z][n]
            cover_ref[row, :] = encode((1.0 - up[3] * clear[3]) * visible)
            return carry

        lax.fori_loop(0, BLK // SUB, some_rows, 0, unroll=2)


def prepare(step, full, x1, x2, rank, angles, slope, shift):
    dep, rows, cols = full.shape
    plane = lambda n: pltpu.VMEM((n, rows, cols), F32)
    return pl.pallas_call(
        lambda *refs: prepare_kernel(step, *refs),
        out_shape=(
            plane(dep), plane(dep), plane(3 * dep), pltpu.VMEM((rows, cols), F32),
            pltpu.VMEM((2, SUB, cols), F32),
        ),
        in_specs=[VMEM] * 3 + [SMEM] * 4,
        out_specs=(VMEM,) * 5,
        scratch_shapes=[
            pltpu.VMEM((2, rows + 2 * PAD, 2 * cols), BF16),
            pltpu.VMEM((4, BLK, cols), F32),
            pltpu.VMEM((2, BLK, 2 * cols), F32),
        ],
        cost_estimate=pl.CostEstimate(flops=10**9, bytes_accessed=10**6, transcendentals=0),
        compiler_params=GRANT,
        name="prepare",
    )(*(near(x) for x in (full, x1, x2)), *(far(x) for x in (rank, angles, slope, shift)))


def shade_kernel(
    full_ref, z1_ref, z2_ref, lit_ref, size_ref, coef_ref, cover_ref, flag_ref,
    image_ref, shade_ref,
):
    _, rows, cols = full_ref.shape
    even_z = lax.rem(lax.axis_index("depth"), 2) == 0
    light_z = flag_ref[0]

    def some_rows(i, carry):
        row = pl.ds(pl.multiple_of(i * SUB, SUB), SUB)
        own = [full_ref[z, row, :].astype(F32) for z in range(4)]
        one = [z1_ref[q, row, :].astype(F32) for q in range(2)]
        two = [z2_ref[q, row, :].astype(F32) for q in range(2)]
        planes = (
            [jnp.where(even_z, two[q], one[q]) for q in range(2)]
            + own
            + [jnp.where(even_z, one[q], two[q]) for q in range(2)]
        )
        shade = []
        for z in range(4):
            gz = (planes[z] - planes[z + 4]) + 8.0 * (planes[z + 3] - planes[z + 1])
            lit = lit_ref[z, row, :] + light_z * gz
            size = size_ref[z, row, :] + gz * gz
            shade.append(0.25 + 0.75 * (jnp.abs(lit) * lax.rsqrt(size)))
        out = []
        for n in range(3):
            part = [shade[z] * coef_ref[3 * z + n, row, :] for z in range(4)]
            out.append(encode((part[0] + part[1]) + (part[2] + part[3])))
        out.append(cover_ref[row, :])
        for half in range(SUB // 8):
            tile = jnp.concatenate([x[half * 8 : half * 8 + 8] for x in out], 0)
            image_ref[i * (SUB // 8) + half] = tile.astype(image_ref.dtype)
        shade_ref[0, row, :] = 0.25 * ((shade[0] + shade[1]) + (shade[2] + shade[3]))
        return carry

    lax.fori_loop(0, rows // SUB, some_rows, 0, unroll=4)


def shade(full, z1, z2, lit, size, coef, cover, flag):
    _, rows, cols = full.shape
    return pl.pallas_call(
        shade_kernel,
        out_shape=(
            pltpu.VMEM((rows // 8, 32, cols), BF16),
            jax.ShapeDtypeStruct((1, rows, cols), F32),
        ),
        in_specs=[VMEM] * 8,
        out_specs=(VMEM, VMEM),
        compiler_params=GRANT,
        name="shade",
    )(*(near(x) for x in (full, z1, z2, lit, size, coef, cover, flag)))


def compose_kernel(part_ref, flag_ref, image_ref):
    slabs, _, cols = part_ref.shape
    ascending = jnp.max(flag_ref[1, 0:8, :]) > 0.5

    def body(i, carry):
        through, red, green, blue = carry
        tile = decode(part_ref[jnp.where(ascending, i, slabs - 1 - i)].astype(F32))
        red = red + through * tile[0:8]
        green = green + through * tile[8:16]
        blue = blue + through * tile[16:24]
        return (through * (1.0 - tile[24:32]), red, green, blue)

    zero = jnp.zeros((8, cols), F32)
    through, red, green, blue = lax.fori_loop(
        0, slabs, body, (jnp.ones((8, cols), F32), zero, zero, zero), unroll=8
    )
    image_ref[0] = red
    image_ref[1] = green
    image_ref[2] = blue
    image_ref[3] = 1.0 - through


def compose(parts, flag):
    return pl.pallas_call(
        compose_kernel,
        out_shape=jax.ShapeDtypeStruct((4, 8, parts.shape[2]), F32),
        in_specs=[VMEM, VMEM],
        out_specs=VMEM,
        compiler_params=GRANT,
        name="compose",
    )(near(parts), near(flag))


def mates(count, start):
    low = range(start, count - 1, 2)
    return [(i, i + 1) for i in low] + [(i + 1, i) for i in low]


def shards(coarse, residual, levels, slab_rank, light_angles, color_slope, color_shift):
    dep = residual.shape[0]
    slabs, tiles = lax.axis_size("depth"), lax.axis_size("tile")
    step = 4.0 / (dep * slabs)
    full, z1, z2, x1, x2 = refine(residual, coarse, levels)
    z1 = lax.ppermute(z1, "depth", mates(slabs, 0))
    z2 = lax.ppermute(z2, "depth", mates(slabs, 1))
    x1 = lax.ppermute(x1, "tile", mates(tiles, 0))
    x2 = lax.ppermute(x2, "tile", mates(tiles, 1))
    ready = prepare(step, full, x1, x2, slab_rank, light_angles, color_slope, color_shift)
    image, mean = shade(full, z1, z2, *ready)
    parts = lax.all_to_all(image, "depth", split_axis=0, concat_axis=0, tiled=True)
    return (compose(parts, ready[-1]), mean)


def solution(mesh):
    placed = (
        P("depth", None, "tile"),
        P("depth", None, "tile"),
        P("depth", None, "tile"),
        P(),
        P(),
        P(),
        P(),
    )
    return jax.shard_map(
        shards,
        mesh=mesh,
        in_specs=placed,
        out_specs=(P(None, "depth", "tile"), P("depth", None, "tile")),
        check_vma=False,
    )
```

```python
import jax
import jax.numpy as jnp
from jax import lax
from jax.experimental import pallas as pl
from jax.experimental.pallas import tpu as pltpu
from jax.sharding import PartitionSpec as P

F32 = jnp.float32
BF16 = jnp.bfloat16
VMEM = pl.BlockSpec(memory_space=pltpu.VMEM)
SMEM = pl.BlockSpec(memory_space=pltpu.SMEM)
NN = (((1,), (0,)), ((), ()))
NT = (((1,), (1,)), ((), ()))
PAD = 64
BLK = 128
SUB = 16


GRANT = pltpu.CompilerParams(vmem_limit_bytes=12 * 2**20)
GAIN = 16.0


def far(x):
    return pltpu.with_memory_space_constraint(x, pltpu.HBM)


def near(x):
    return pltpu.with_memory_space_constraint(x, pltpu.VMEM)


def dot(a, b, dims=NN):
    return lax.dot_general(a, b, dims, preferred_element_type=F32)


def iota2(shape):
    return (
        lax.broadcasted_iota(jnp.int32, shape, 0),
        lax.broadcasted_iota(jnp.int32, shape, 1),
    )


def repeater(out, inner):
    r, c = iota2((out, inner))
    return jnp.where(r // (out // inner) == c, 1.0, 0.0).astype(BF16)


def stencil(offset):
    w = jnp.where(offset == -2, 1.0, jnp.where(offset == -1, -8.0, 0.0))
    return jnp.where(offset == 1, 8.0, jnp.where(offset == 2, -1.0, w))


def encode(x):
    x = x * GAIN
    x = x * x
    return x * x


def decode(x):
    for _ in range(2):
        x = x * lax.rsqrt(jnp.maximum(x, 1e-37))
    return x * (1.0 / GAIN)


def refine_kernel(
    res_ref, coarse_ref, level_ref, full_ref, z1_ref, z2_ref, x1_ref, x2_ref
):
    dep, rows, cols = res_ref.shape
    half = coarse_ref.shape[2]
    even_z = lax.rem(lax.axis_index("depth"), 2) == 0
    even_x = lax.rem(lax.axis_index("tile"), 2) == 0
    widen2 = repeater(cols, coarse_ref.shape[1])
    widen4 = repeater(cols, level_ref.shape[0])
    lev = dot(widen4, level_ref[...].astype(F32).astype(BF16)).astype(BF16)
    scale = 0.5 * dot(repeater(rows, lev.shape[1]), lev, NT)
    tall2 = repeater(256, 128)
    k, c = iota2((16, cols))
    edges = jnp.zeros((16, rows), F32)
    for zc in range(dep // 2):
        wide = dot(widen2, coarse_ref[zc]).astype(BF16)
        lifted = [dot(tall2, wide[:, b * 128 : (b + 1) * 128], NT) for b in range(half // 128)]
        for z in (2 * zc, 2 * zc + 1):
            for b in range(half // 128):
                part = pl.ds(b * 256, 256)
                full_ref[z, part, :] = (
                    lifted[b] + scale[b * 256 : (b + 1) * 256] * res_ref[z, part, :].astype(F32)
                ).astype(BF16)
            col = jnp.where(k < 8, k - 2 * z + cols - 2, k - 8 - 2 * z)
            mine = (k % 8) // 2 == z
            pick = jnp.where(mine & (col == c), 1.0, 0.0).astype(BF16)
            edges = edges + dot(pick, full_ref[z], NT)
    for p in range(2):
        z1_ref[p] = jnp.where(even_z, full_ref[2 + p], full_ref[p])
        z2_ref[p] = jnp.where(even_z, full_ref[p], full_ref[2 + p])
    last, first = edges[0:8], edges[8:16]
    x1_ref[...] = jnp.where(even_x, last, first).astype(BF16)
    x2_ref[...] = jnp.where(even_x, first, last).astype(BF16)


def refine(residual, coarse, levels):
    dep, rows, cols = residual.shape
    plane = pltpu.VMEM((2, rows, cols), BF16)
    edge = pltpu.VMEM((2 * dep, rows), BF16)
    return pl.pallas_call(
        refine_kernel,
        out_shape=(pltpu.VMEM((dep, rows, cols), BF16), plane, plane, edge, edge),
        in_specs=[VMEM] * 3,
        out_specs=(VMEM,) * 5,
        cost_estimate=pl.CostEstimate(flops=10**8, bytes_accessed=10**6, transcendentals=0),
        compiler_params=GRANT,
        name="refine",
    )(*(far(x) for x in (residual, jnp.swapaxes(coarse, 1, 2), jnp.swapaxes(levels[0], 0, 1))))


def prepare_kernel(
    step, full_ref, x1_ref, x2_ref, rank_ref, angle_ref, slope_ref, shift_ref,
    lit_ref, size_ref, coef_ref, cover_ref, flag_ref, pair, gx_ref, gy_ref,
):
    dep, rows, cols = full_ref.shape
    slabs = rank_ref.shape[0]
    even_x = lax.rem(lax.axis_index("tile"), 2) == 0
    ascending = rank_ref[0] < rank_ref[slabs - 1]
    visible = jnp.where(rank_ref[lax.axis_index("depth")] >= 0, 1.0, 0.0).astype(F32)
    azimuth = jnp.full((SUB, cols), angle_ref[0], F32)
    elevation = jnp.full((SUB, cols), angle_ref[1], F32)
    light_y = jnp.cos(elevation) * jnp.sin(azimuth)
    light_x = jnp.cos(elevation) * jnp.cos(azimuth)
    slope = [0.5 * slope_ref[k] for k in range(3)]
    shift = [0.5 * shift_ref[k] for k in range(3)]
    flag_ref[0] = jnp.sin(elevation)
    flag_ref[1] = jnp.full((SUB, cols), jnp.where(ascending, 1.0, 0.0), F32)

    zero = jnp.zeros((PAD, 2 * cols), BF16)
    for p in range(2):
        pair[p, 0:PAD, :] = zero
        pair[p, PAD + rows :, :] = zero
        for q in range(2):
            pair[p, PAD : PAD + rows, q * cols : (q + 1) * cols] = full_ref[2 * p + q]

    r, c = iota2((cols, cols))
    across = stencil(r - c).astype(BF16)
    r, c = iota2((BLK, BLK + 2 * PAD))
    along = stencil(c - PAD - r).astype(BF16)
    k, c = iota2((16, cols))
    spot = jnp.where(k < 8, k % 2 - 2, cols + k % 2)
    beside = [
        jnp.where((k % 8) // 2 == z, stencil(spot - c), 0.0).astype(BF16) for z in range(4)
    ]
    x1, x2 = x1_ref[...].astype(F32), x2_ref[...].astype(F32)
    columns = jnp.concatenate([jnp.where(even_x, x2, x1), jnp.where(even_x, x1, x2)], 0)
    columns = columns.T.astype(BF16)

    for b in range(rows // BLK):
        base = b * BLK
        for p in range(2):
            gy_ref[p] = dot(along, pair[p, base : base + BLK + 2 * PAD, :])
            for q in range(2):
                z = 2 * p + q
                gx_ref[z] = dot(full_ref[z, base : base + BLK, :], across) + dot(
                    columns[base : base + BLK], beside[z]
                )

        def some_rows(i, carry, base=base):
            at = pl.ds(pl.multiple_of(i * SUB, SUB), SUB)
            row = pl.ds(pl.multiple_of(base + i * SUB, SUB), SUB)
            clear, color = [], []
            for z in range(4):
                v = full_ref[z, row, :].astype(F32)
                gy = gy_ref[z // 2, at, (z % 2) * cols : (z % 2 + 1) * cols]
                gx = gx_ref[z, at, :]
                lit_ref[z, row, :] = light_y * gy + light_x * gx
                size_ref[z, row, :] = gy * gy + gx * gx + 144.0
                extinct = 2.0 + 2.0 * jnp.tanh(1.5 * v - 2.25)
                clear.append(jnp.exp(-step * extinct))
                color.append([0.5 + 0.5 * jnp.tanh(slope[n] * v + shift[n]) for n in range(3)])
            up = [None, clear[0], clear[0] * clear[1], None]
            up[3] = up[2] * clear[2]
            down = [None, None, clear[3], None]
            down[1] = clear[3] * clear[2]
            down[0] = down[1] * clear[1]
            before = [
                jnp.where(ascending, 1.0, down[0]),
                jnp.where(ascending, up[1], down[1]),
                jnp.where(ascending, up[2], down[2]),
                jnp.where(ascending, up[3], 1.0),
            ]
            for z in range(4):
                weight = before[z] * (1.0 - clear[z]) * visible
                for n in range(3):
                    coef_ref[3 * z + n, row, :] = weight * color[z][n]
            cover_ref[row, :] = encode((1.0 - up[3] * clear[3]) * visible)
            return carry

        lax.fori_loop(0, BLK // SUB, some_rows, 0, unroll=2)


def prepare(step, full, x1, x2, rank, angles, slope, shift):
    dep, rows, cols = full.shape
    plane = lambda n: pltpu.VMEM((n, rows, cols), F32)
    return pl.pallas_call(
        lambda *refs: prepare_kernel(step, *refs),
        out_shape=(
            plane(dep), plane(dep), plane(3 * dep), pltpu.VMEM((rows, cols), F32),
            pltpu.VMEM((2, SUB, cols), F32),
        ),
        in_specs=[VMEM] * 3 + [SMEM] * 4,
        out_specs=(VMEM,) * 5,
        scratch_shapes=[
            pltpu.VMEM((2, rows + 2 * PAD, 2 * cols), BF16),
            pltpu.VMEM((4, BLK, cols), F32),
            pltpu.VMEM((2, BLK, 2 * cols), F32),
        ],
        cost_estimate=pl.CostEstimate(flops=10**9, bytes_accessed=10**6, transcendentals=0),
        compiler_params=GRANT,
        name="prepare",
    )(*(near(x) for x in (full, x1, x2)), *(far(x) for x in (rank, angles, slope, shift)))


def shade_kernel(
    full_ref, z1_ref, z2_ref, lit_ref, size_ref, coef_ref, cover_ref, flag_ref,
    image_ref, shade_ref,
):
    _, rows, cols = full_ref.shape
    even_z = lax.rem(lax.axis_index("depth"), 2) == 0
    light_z = flag_ref[0]

    def some_rows(i, carry):
        row = pl.ds(pl.multiple_of(i * SUB, SUB), SUB)
        own = [full_ref[z, row, :].astype(F32) for z in range(4)]
        one = [z1_ref[q, row, :].astype(F32) for q in range(2)]
        two = [z2_ref[q, row, :].astype(F32) for q in range(2)]
        planes = (
            [jnp.where(even_z, two[q], one[q]) for q in range(2)]
            + own
            + [jnp.where(even_z, one[q], two[q]) for q in range(2)]
        )
        shade = []
        for z in range(4):
            gz = (planes[z] - planes[z + 4]) + 8.0 * (planes[z + 3] - planes[z + 1])
            lit = lit_ref[z, row, :] + light_z * gz
            size = size_ref[z, row, :] + gz * gz
            shade.append(0.25 + 0.75 * (jnp.abs(lit) * lax.rsqrt(size)))
        out = []
        for n in range(3):
            part = [shade[z] * coef_ref[3 * z + n, row, :] for z in range(4)]
            out.append(encode((part[0] + part[1]) + (part[2] + part[3])))
        out.append(cover_ref[row, :])
        for half in range(SUB // 8):
            tile = jnp.concatenate([x[half * 8 : half * 8 + 8] for x in out], 0)
            image_ref[i * (SUB // 8) + half] = tile.astype(image_ref.dtype)
        shade_ref[0, row, :] = 0.25 * ((shade[0] + shade[1]) + (shade[2] + shade[3]))
        return carry

    lax.fori_loop(0, rows // SUB, some_rows, 0, unroll=4)


def shade(full, z1, z2, lit, size, coef, cover, flag):
    _, rows, cols = full.shape
    return pl.pallas_call(
        shade_kernel,
        out_shape=(
            pltpu.VMEM((rows // 8, 32, cols), BF16),
            jax.ShapeDtypeStruct((1, rows, cols), F32),
        ),
        in_specs=[VMEM] * 8,
        out_specs=(VMEM, VMEM),
        compiler_params=GRANT,
        name="shade",
    )(*(near(x) for x in (full, z1, z2, lit, size, coef, cover, flag)))


def compose_kernel(part_ref, flag_ref, image_ref):
    slabs, _, cols = part_ref.shape
    ascending = jnp.max(flag_ref[1, 0:8, :]) > 0.5

    def body(i, carry):
        through, red, green, blue = carry
        tile = decode(part_ref[jnp.where(ascending, i, slabs - 1 - i)].astype(F32))
        red = red + through * tile[0:8]
        green = green + through * tile[8:16]
        blue = blue + through * tile[16:24]
        return (through * (1.0 - tile[24:32]), red, green, blue)

    zero = jnp.zeros((8, cols), F32)
    through, red, green, blue = lax.fori_loop(
        0, slabs, body, (jnp.ones((8, cols), F32), zero, zero, zero), unroll=8
    )
    image_ref[0] = red
    image_ref[1] = green
    image_ref[2] = blue
    image_ref[3] = 1.0 - through


def compose(parts, flag):
    return pl.pallas_call(
        compose_kernel,
        out_shape=jax.ShapeDtypeStruct((4, 8, parts.shape[2]), F32),
        in_specs=[VMEM, VMEM],
        out_specs=VMEM,
        compiler_params=GRANT,
        name="compose",
    )(near(parts), near(flag))


def mates(count, start):
    low = range(start, count - 1, 2)
    return [(i, i + 1) for i in low] + [(i + 1, i) for i in low]


def shards(coarse, residual, levels, slab_rank, light_angles, color_slope, color_shift):
    dep = residual.shape[0]
    slabs, tiles = lax.axis_size("depth"), lax.axis_size("tile")
    step = 4.0 / (dep * slabs)
    full, z1, z2, x1, x2 = refine(residual, coarse, levels)
    x2 = lax.ppermute(x2, "tile", mates(tiles, 1))
    z1 = lax.ppermute(z1, "depth", mates(slabs, 0))
    z2 = lax.ppermute(z2, "depth", mates(slabs, 1))
    x1 = lax.ppermute(x1, "tile", mates(tiles, 0))
    ready = prepare(step, full, x1, x2, slab_rank, light_angles, color_slope, color_shift)
    image, mean = shade(full, z1, z2, *ready)
    parts = lax.all_to_all(image, "depth", split_axis=0, concat_axis=0, tiled=True)
    return (compose(parts, ready[-1]), mean)


def solution(mesh):
    placed = (
        P("depth", None, "tile"),
        P("depth", None, "tile"),
        P("depth", None, "tile"),
        P(),
        P(),
        P(),
        P(),
    )
    return jax.shard_map(
        shards,
        mesh=mesh,
        in_specs=placed,
        out_specs=(P(None, "depth", "tile"), P("depth", None, "tile")),
        check_vma=False,
    )
```

```python
import functools

import jax
import jax.numpy as jnp
from jax import lax
from jax.experimental import pallas as pl
from jax.experimental.pallas import tpu as pltpu
from jax.sharding import PartitionSpec as P

F32 = jnp.float32
BF16 = jnp.bfloat16
VMEM = pl.BlockSpec(memory_space=pltpu.VMEM)
SMEM = pl.BlockSpec(memory_space=pltpu.SMEM)
NN = (((1,), (0,)), ((), ()))
NT = (((1,), (1,)), ((), ()))
PAD = 64
BLK = 128
SUB = 16


GRANT = pltpu.CompilerParams(vmem_limit_bytes=12 * 2**20)
GAIN = 16.0


def far(x):
    return pltpu.with_memory_space_constraint(x, pltpu.HBM)


def near(x):
    return pltpu.with_memory_space_constraint(x, pltpu.VMEM)


def dot(a, b, dims=NN):
    return lax.dot_general(a, b, dims, preferred_element_type=F32)


def iota2(shape):
    return (
        lax.broadcasted_iota(jnp.int32, shape, 0),
        lax.broadcasted_iota(jnp.int32, shape, 1),
    )


def repeater(out, inner):
    r, c = iota2((out, inner))
    return jnp.where(r // (out // inner) == c, 1.0, 0.0).astype(BF16)


def stencil(offset):
    w = jnp.where(offset == -2, 1.0, jnp.where(offset == -1, -8.0, 0.0))
    return jnp.where(offset == 1, 8.0, jnp.where(offset == 2, -1.0, w))


def seat(d):
    y, x, z = d >> 4, (d >> 2) & 3, d & 3
    return z * 16 + (3 - y) * 4 + (3 - x)


def encode(x):
    x = x * GAIN
    x = x * x
    return x * x


def decode(x):
    for _ in range(2):
        x = x * lax.rsqrt(jnp.maximum(x, 1e-37))
    return x * (1.0 / GAIN)


def refine_kernel(
    res_ref, coarse_ref, level_ref, full_ref, z1_ref, z2_ref, x1_ref, x2_ref
):
    dep, rows, cols = res_ref.shape
    half = coarse_ref.shape[2]
    even_z = lax.rem(lax.axis_index("depth"), 2) == 0
    even_x = lax.rem(lax.axis_index("tile"), 2) == 0
    widen2 = repeater(cols, coarse_ref.shape[1])
    widen4 = repeater(cols, level_ref.shape[0])
    lev = dot(widen4, level_ref[...].astype(F32).astype(BF16)).astype(BF16)
    scale = 0.5 * dot(repeater(rows, lev.shape[1]), lev, NT)
    tall2 = repeater(256, 128)
    k, c = iota2((16, cols))
    edges = jnp.zeros((16, rows), F32)
    wide = [dot(widen2, coarse_ref[zc]).astype(BF16) for zc in range(dep // 2)]
    for b in range(half // 128):
        part = pl.ds(b * 256, 256)
        packs = []
        for zc in range(dep // 2):
            lifted = dot(tall2, wide[zc][:, b * 128 : (b + 1) * 128], NT)
            both = [
                lifted + scale[b * 256 : (b + 1) * 256] * res_ref[z, part, :].astype(F32)
                for z in (2 * zc, 2 * zc + 1)
            ]
            for q in range(2):
                full_ref[2 * zc + q, part, :] = both[q].astype(BF16)
            packs.append(
                jnp.concatenate([v.reshape(32, 8, cols) for v in both], 1).astype(BF16)
            )
        group = pl.ds(b * 32, 32)
        z1_ref[group] = jnp.where(even_z, packs[1], packs[0])
        z2_ref[group] = jnp.where(even_z, packs[0], packs[1])
    for z in range(dep):
        col = jnp.where(k < 8, k - 2 * z + cols - 2, k - 8 - 2 * z)
        mine = (k % 8) // 2 == z
        pick = jnp.where(mine & (col == c), 1.0, 0.0).astype(BF16)
        edges = edges + dot(pick, full_ref[z], NT)
    last, first = edges[0:8], edges[8:16]
    x1_ref[...] = jnp.where(even_x, last, first).astype(BF16)
    x2_ref[...] = jnp.where(even_x, first, last).astype(BF16)


def refine(residual, coarse, levels):
    dep, rows, cols = residual.shape
    plane = pltpu.VMEM((rows // 8, 16, cols), BF16)
    edge = pltpu.VMEM((2 * dep, rows), BF16)
    return pl.pallas_call(
        refine_kernel,
        out_shape=(pltpu.VMEM((dep, rows, cols), BF16), plane, plane, edge, edge),
        in_specs=[VMEM] * 3,
        out_specs=(VMEM,) * 5,
        cost_estimate=pl.CostEstimate(flops=10**8, bytes_accessed=10**6, transcendentals=0),
        compiler_params=GRANT,
        name="refine",
    )(*(far(x) for x in (residual, jnp.swapaxes(coarse, 1, 2), jnp.swapaxes(levels[0], 0, 1))))


def prepare_kernel(
    step, full_ref, x1_ref, x2_ref, rank_ref, angle_ref, slope_ref, shift_ref,
    lit_ref, size_ref, part_ref, coef_ref, cover_ref, flag_ref, pair, gx_ref, gy_ref,
):
    dep, rows, cols = full_ref.shape
    slabs = rank_ref.shape[0]
    even_x = lax.rem(lax.axis_index("tile"), 2) == 0
    ascending = rank_ref[0] < rank_ref[slabs - 1]
    visible = jnp.where(rank_ref[lax.axis_index("depth")] >= 0, 1.0, 0.0).astype(F32)
    azimuth = jnp.full((SUB, cols), angle_ref[0], F32)
    elevation = jnp.full((SUB, cols), angle_ref[1], F32)
    light_y = jnp.cos(elevation) * jnp.sin(azimuth)
    light_x = jnp.cos(elevation) * jnp.cos(azimuth)
    slope = [0.5 * slope_ref[k] for k in range(3)]
    shift = [0.5 * shift_ref[k] for k in range(3)]
    flag_ref[0] = jnp.sin(elevation)
    flag_ref[1] = jnp.full((SUB, cols), jnp.where(ascending, 1.0, 0.0), F32)

    zero = jnp.zeros((PAD, 2 * cols), BF16)
    for p in range(2):
        pair[p, 0:PAD, :] = zero
        pair[p, PAD + rows :, :] = zero
        for q in range(2):
            pair[p, PAD : PAD + rows, q * cols : (q + 1) * cols] = full_ref[2 * p + q]

    r, c = iota2((cols, cols))
    across = stencil(r - c).astype(BF16)
    r, c = iota2((BLK, BLK + 2 * PAD))
    along = stencil(c - PAD - r).astype(BF16)
    k, c = iota2((16, cols))
    spot = jnp.where(k < 8, k % 2 - 2, cols + k % 2)
    beside = [
        jnp.where((k % 8) // 2 == z, stencil(spot - c), 0.0).astype(BF16) for z in range(4)
    ]
    x1, x2 = x1_ref[...].astype(F32), x2_ref[...].astype(F32)
    columns = jnp.concatenate([jnp.where(even_x, x2, x1), jnp.where(even_x, x1, x2)], 0)
    columns = columns.T.astype(BF16)

    for b in range(rows // BLK):
        base = b * BLK
        for p in range(2):
            gy_ref[p] = dot(along, pair[p, base : base + BLK + 2 * PAD, :])
            for q in range(2):
                z = 2 * p + q
                gx_ref[z] = dot(full_ref[z, base : base + BLK, :], across) + dot(
                    columns[base : base + BLK], beside[z]
                )

        def some_rows(i, carry, base=base):
            at = pl.ds(pl.multiple_of(i * SUB, SUB), SUB)
            row = pl.ds(pl.multiple_of(base + i * SUB, SUB), SUB)
            own = [full_ref[z, row, :].astype(F32) for z in range(4)]
            part_ref[0, row, :] = 8.0 * own[1] - own[2]
            part_ref[1, row, :] = 8.0 * (own[2] - own[0]) - own[3]
            part_ref[2, row, :] = 8.0 * (own[3] - own[1]) + own[0]
            part_ref[3, row, :] = own[1] - 8.0 * own[2]
            clear, color = [], []
            for z in range(4):
                v = own[z]
                gy = gy_ref[z // 2, at, (z % 2) * cols : (z % 2 + 1) * cols]
                gx = gx_ref[z, at, :]
                lit_ref[z, row, :] = light_y * gy + light_x * gx
                size_ref[z, row, :] = gy * gy + gx * gx + 144.0
                extinct = 2.0 + 2.0 * jnp.tanh(1.5 * v - 2.25)
                clear.append(jnp.exp(-step * extinct))
                color.append([0.5 + 0.5 * jnp.tanh(slope[n] * v + shift[n]) for n in range(3)])
            up = [None, clear[0], clear[0] * clear[1], None]
            up[3] = up[2] * clear[2]
            down = [None, None, clear[3], None]
            down[1] = clear[3] * clear[2]
            down[0] = down[1] * clear[1]
            before = [
                jnp.where(ascending, 1.0, down[0]),
                jnp.where(ascending, up[1], down[1]),
                jnp.where(ascending, up[2], down[2]),
                jnp.where(ascending, up[3], 1.0),
            ]
            for z in range(4):
                weight = before[z] * (1.0 - clear[z]) * visible
                for n in range(3):
                    coef_ref[3 * z + n, row, :] = weight * color[z][n]
            cover_ref[row, :] = encode((1.0 - up[3] * clear[3]) * visible)
            return carry

        lax.fori_loop(0, BLK // SUB, some_rows, 0, unroll=2)


def prepare(step, full, x1, x2, rank, angles, slope, shift):
    dep, rows, cols = full.shape
    plane = lambda n: pltpu.VMEM((n, rows, cols), F32)
    return pl.pallas_call(
        lambda *refs: prepare_kernel(step, *refs),
        out_shape=(
            plane(dep), plane(dep), plane(dep), plane(3 * dep), pltpu.VMEM((rows, cols), F32),
            pltpu.VMEM((2, SUB, cols), F32),
        ),
        in_specs=[VMEM] * 3 + [SMEM] * 4,
        out_specs=(VMEM,) * 6,
        scratch_shapes=[
            pltpu.VMEM((2, rows + 2 * PAD, 2 * cols), BF16),
            pltpu.VMEM((4, BLK, cols), F32),
            pltpu.VMEM((2, BLK, 2 * cols), F32),
        ],
        cost_estimate=pl.CostEstimate(flops=10**9, bytes_accessed=10**6, transcendentals=0),
        compiler_params=GRANT,
        name="prepare",
    )(*(near(x) for x in (full, x1, x2)), *(far(x) for x in (rank, angles, slope, shift)))


def shade_kernel(
    z1_ref, z2_ref, lit_ref, size_ref, part_ref, coef_ref, cover_ref, flag_ref,
    image_ref, mean_ref,
):
    cols = lit_ref.shape[2]
    even_z = lax.rem(lax.axis_index("depth"), 2) == 0
    light_z = flag_ref[0, 0:8, :]

    def group(i, carry, start=0, z1_ref=z1_ref):
        r = start + i
        row = pl.ds(pl.multiple_of(8 * r, 8), 8)
        one, two = z1_ref[i].astype(F32), z2_ref[r].astype(F32)
        low = jnp.where(even_z, two, one)
        high = jnp.where(even_z, one, two)
        part = [part_ref[z, row, :] for z in range(4)]
        gz = (
            part[0] + (low[0:8] - 8.0 * low[8:16]),
            part[1] + low[8:16],
            part[2] - high[0:8],
            part[3] + (8.0 * high[0:8] - high[8:16]),
        )
        shade = []
        for z in range(4):
            lit = lit_ref[z, row, :] + light_z * gz[z]
            size = size_ref[z, row, :] + gz[z] * gz[z]
            shade.append(0.25 + 0.75 * (jnp.abs(lit) * lax.rsqrt(size)))
        out = []
        for n in range(3):
            p = [shade[z] * coef_ref[3 * z + n, row, :] for z in range(4)]
            out.append(encode((p[0] + p[1]) + (p[2] + p[3])))
        out.append(cover_ref[row, :])
        image_ref[seat(r)] = jnp.concatenate(out, 0).astype(BF16)
        mean_ref[0, row, :] = 0.25 * ((shade[0] + shade[1]) + (shade[2] + shade[3]))
        return carry

    start = 0
    for ref in (z1_ref,):
        body = functools.partial(group, start=start, z1_ref=ref)
        lax.fori_loop(0, ref.shape[0], body, 0, unroll=8)
        start += ref.shape[0]


def shade(z1, z2, ready):
    _, rows, cols = ready[0].shape
    return pl.pallas_call(
        shade_kernel,
        out_shape=(
            pltpu.VMEM((rows // 8, 32, cols), BF16),
            jax.ShapeDtypeStruct((1, rows, cols), F32),
        ),
        in_specs=[VMEM] * 8,
        out_specs=(VMEM, VMEM),
        compiler_params=GRANT,
        name="shade",
    )(*(near(x) for x in (z1, z2, *ready)))


def compose_kernel(part_ref, flag_ref, image_ref):
    slabs, _, cols = part_ref.shape
    ascending = jnp.max(flag_ref[1, 0:8, :]) > 0.5

    def body(i, carry):
        through, red, green, blue = carry
        tile = decode(part_ref[seat(jnp.where(ascending, i, slabs - 1 - i))].astype(F32))
        red = red + through * tile[0:8]
        green = green + through * tile[8:16]
        blue = blue + through * tile[16:24]
        return (through * (1.0 - tile[24:32]), red, green, blue)

    zero = jnp.zeros((8, cols), F32)
    through, red, green, blue = lax.fori_loop(
        0, slabs, body, (jnp.ones((8, cols), F32), zero, zero, zero), unroll=8
    )
    image_ref[0] = red
    image_ref[1] = green
    image_ref[2] = blue
    image_ref[3] = 1.0 - through


def compose(parts, flag):
    return pl.pallas_call(
        compose_kernel,
        out_shape=jax.ShapeDtypeStruct((4, 8, parts.shape[2]), F32),
        in_specs=[VMEM, VMEM],
        out_specs=VMEM,
        compiler_params=GRANT,
        name="compose",
    )(near(parts), near(flag))


def mates(count, start):
    low = range(start, count - 1, 2)
    return [(i, i + 1) for i in low] + [(i + 1, i) for i in low]


def shards(coarse, residual, levels, slab_rank, light_angles, color_slope, color_shift):
    dep = residual.shape[0]
    slabs, tiles = lax.axis_size("depth"), lax.axis_size("tile")
    step = 4.0 / (dep * slabs)
    full, z1, z2, x1, x2 = refine(residual, coarse, levels)
    z1 = lax.ppermute(z1, "depth", mates(slabs, 0))
    z2 = lax.ppermute(z2, "depth", mates(slabs, 1))
    x1 = lax.ppermute(x1, "tile", mates(tiles, 0))
    x2 = lax.ppermute(x2, "tile", mates(tiles, 1))
    ready = prepare(step, full, x1, x2, slab_rank, light_angles, color_slope, color_shift)
    image, mean = shade(z1, z2, ready)
    order = sorted(range(slabs), key=seat)
    parts = lax.all_to_all(
        image, "depth", split_axis=0, concat_axis=0, tiled=True, axis_index_groups=[order]
    )
    return (compose(parts, ready[-1]), mean)


def solution(mesh):
    placed = (
        P("depth", None, "tile"),
        P("depth", None, "tile"),
        P("depth", None, "tile"),
        P(),
        P(),
        P(),
        P(),
    )
    return jax.shard_map(
        shards,
        mesh=mesh,
        in_specs=placed,
        out_specs=(P(None, "depth", "tile"), P("depth", None, "tile")),
        check_vma=False,
    )
```

```python
import functools

import jax
import jax.numpy as jnp
from jax import lax
from jax.experimental import pallas as pl
from jax.experimental.pallas import tpu as pltpu
from jax.sharding import PartitionSpec as P

F32 = jnp.float32
BF16 = jnp.bfloat16
VMEM = pl.BlockSpec(memory_space=pltpu.VMEM)
SMEM = pl.BlockSpec(memory_space=pltpu.SMEM)
NN = (((1,), (0,)), ((), ()))
NT = (((1,), (1,)), ((), ()))
PAD = 64
BLK = 128
SUB = 16


GRANT = pltpu.CompilerParams(vmem_limit_bytes=12 * 2**20)
GAIN = 16.0


def far(x):
    return pltpu.with_memory_space_constraint(x, pltpu.HBM)


def near(x):
    return pltpu.with_memory_space_constraint(x, pltpu.VMEM)


def dot(a, b, dims=NN):
    return lax.dot_general(a, b, dims, preferred_element_type=F32)


def iota2(shape):
    return (
        lax.broadcasted_iota(jnp.int32, shape, 0),
        lax.broadcasted_iota(jnp.int32, shape, 1),
    )


def repeater(out, inner):
    r, c = iota2((out, inner))
    return jnp.where(r // (out // inner) == c, 1.0, 0.0).astype(BF16)


def stencil(offset):
    w = jnp.where(offset == -2, 1.0, jnp.where(offset == -1, -8.0, 0.0))
    return jnp.where(offset == 1, 8.0, jnp.where(offset == 2, -1.0, w))


def seat(d):
    y, x, z = d >> 4, (d >> 2) & 3, d & 3
    return z * 16 + (3 - y) * 4 + (3 - x)


def encode(x):
    x = x * GAIN
    x = x * x
    return x * x


def decode(x):
    for _ in range(2):
        x = x * lax.rsqrt(jnp.maximum(x, 1e-37))
    return x * (1.0 / GAIN)


def refine_kernel(
    res_ref, coarse_ref, level_ref, full_ref, z1_ref, z2_ref, x1_ref, x2_ref
):
    dep, rows, cols = res_ref.shape
    half = coarse_ref.shape[2]
    even_z = lax.rem(lax.axis_index("depth"), 2) == 1
    even_x = lax.rem(lax.axis_index("tile"), 2) == 0
    widen2 = repeater(cols, coarse_ref.shape[1])
    widen4 = repeater(cols, level_ref.shape[0])
    lev = dot(widen4, level_ref[...].astype(F32).astype(BF16)).astype(BF16)
    scale = 0.5 * dot(repeater(rows, lev.shape[1]), lev, NT)
    tall2 = repeater(256, 128)
    k, c = iota2((16, cols))
    edges = jnp.zeros((16, rows), F32)
    wide = [dot(widen2, coarse_ref[zc]).astype(BF16) for zc in range(dep // 2)]
    for b in range(half // 128):
        part = pl.ds(b * 256, 256)
        packs = []
        for zc in range(dep // 2):
            lifted = dot(tall2, wide[zc][:, b * 128 : (b + 1) * 128], NT)
            both = [
                lifted + scale[b * 256 : (b + 1) * 256] * res_ref[z, part, :].astype(F32)
                for z in (2 * zc, 2 * zc + 1)
            ]
            for q in range(2):
                full_ref[2 * zc + q, part, :] = both[q].astype(BF16)
            packs.append(
                jnp.concatenate([v.reshape(32, 8, cols) for v in both], 1).astype(BF16)
            )
        group = pl.ds(b * 32, 32)
        z1_ref[group] = jnp.where(even_z, packs[1], packs[0])
        z2_ref[group] = jnp.where(even_z, packs[0], packs[1])
    for z in range(dep):
        col = jnp.where(k < 8, k - 2 * z + cols - 2, k - 8 - 2 * z)
        mine = (k % 8) // 2 == z
        pick = jnp.where(mine & (col == c), 1.0, 0.0).astype(BF16)
        edges = edges + dot(pick, full_ref[z], NT)
    last, first = edges[0:8], edges[8:16]
    x1_ref[...] = jnp.where(even_x, last, first).astype(BF16)
    x2_ref[...] = jnp.where(even_x, first, last).astype(BF16)


def refine(residual, coarse, levels):
    dep, rows, cols = residual.shape
    plane = pltpu.VMEM((rows // 8, 16, cols), BF16)
    edge = pltpu.VMEM((2 * dep, rows), BF16)
    return pl.pallas_call(
        refine_kernel,
        out_shape=(pltpu.VMEM((dep, rows, cols), BF16), plane, plane, edge, edge),
        in_specs=[VMEM] * 3,
        out_specs=(VMEM,) * 5,
        cost_estimate=pl.CostEstimate(flops=10**8, bytes_accessed=10**6, transcendentals=0),
        compiler_params=GRANT,
        name="refine",
    )(*(far(x) for x in (residual, jnp.swapaxes(coarse, 1, 2), jnp.swapaxes(levels[0], 0, 1))))


def prepare_kernel(
    step, full_ref, rank_ref, angle_ref, slope_ref, shift_ref,
    lit_ref, size_ref, part_ref, coef_ref, cover_ref, flag_ref, gx_ref, pair, gy_ref,
):
    dep, rows, cols = full_ref.shape
    slabs = rank_ref.shape[0]
    ascending = rank_ref[0] < rank_ref[slabs - 1]
    visible = jnp.where(rank_ref[lax.axis_index("depth")] >= 0, 1.0, 0.0).astype(F32)
    azimuth = jnp.full((SUB, cols), angle_ref[0], F32)
    elevation = jnp.full((SUB, cols), angle_ref[1], F32)
    light_y = jnp.cos(elevation) * jnp.sin(azimuth)
    light_x = jnp.cos(elevation) * jnp.cos(azimuth)
    slope = [0.5 * slope_ref[k] for k in range(3)]
    shift = [0.5 * shift_ref[k] for k in range(3)]
    flag_ref[0] = jnp.sin(elevation)
    flag_ref[1] = jnp.full((SUB, cols), jnp.where(ascending, 1.0, 0.0), F32)
    flag_ref[2] = light_x

    zero = jnp.zeros((PAD, 2 * cols), BF16)
    for p in range(2):
        pair[p, 0:PAD, :] = zero
        pair[p, PAD + rows :, :] = zero
        for q in range(2):
            pair[p, PAD : PAD + rows, q * cols : (q + 1) * cols] = full_ref[2 * p + q]

    r, c = iota2((cols, cols))
    across = stencil(r - c).astype(BF16)
    r, c = iota2((BLK, BLK + 2 * PAD))
    along = stencil(c - PAD - r).astype(BF16)
    for b in range(rows // BLK):
        base = b * BLK
        for p in range(2):
            gy_ref[p] = dot(along, pair[p, base : base + BLK + 2 * PAD, :])
            for q in range(2):
                z = 2 * p + q
                gx_ref[z, base : base + BLK, :] = dot(full_ref[z, base : base + BLK, :], across)

        def some_rows(i, carry, base=base):
            at = pl.ds(pl.multiple_of(i * SUB, SUB), SUB)
            row = pl.ds(pl.multiple_of(base + i * SUB, SUB), SUB)
            own = [full_ref[z, row, :].astype(F32) for z in range(4)]
            part_ref[0, row, :] = 8.0 * own[1] - own[2]
            part_ref[1, row, :] = 8.0 * (own[2] - own[0]) - own[3]
            part_ref[2, row, :] = 8.0 * (own[3] - own[1]) + own[0]
            part_ref[3, row, :] = own[1] - 8.0 * own[2]
            clear, color = [], []
            for z in range(4):
                v = own[z]
                gy = gy_ref[z // 2, at, (z % 2) * cols : (z % 2 + 1) * cols]
                gx = gx_ref[z, row, :]
                lit_ref[z, row, :] = light_y * gy + light_x * gx
                size_ref[z, row, :] = gy * gy + gx * gx + 144.0
                extinct = 2.0 + 2.0 * jnp.tanh(1.5 * v - 2.25)
                clear.append(jnp.exp(-step * extinct))
                color.append([0.5 + 0.5 * jnp.tanh(slope[n] * v + shift[n]) for n in range(3)])
            up = [None, clear[0], clear[0] * clear[1], None]
            up[3] = up[2] * clear[2]
            down = [None, None, clear[3], None]
            down[1] = clear[3] * clear[2]
            down[0] = down[1] * clear[1]
            before = [
                jnp.where(ascending, 1.0, down[0]),
                jnp.where(ascending, up[1], down[1]),
                jnp.where(ascending, up[2], down[2]),
                jnp.where(ascending, up[3], 1.0),
            ]
            for z in range(4):
                weight = before[z] * (1.0 - clear[z]) * visible
                for n in range(3):
                    coef_ref[3 * z + n, row, :] = weight * color[z][n]
            cover_ref[row, :] = encode((1.0 - up[3] * clear[3]) * visible)
            return carry

        lax.fori_loop(0, BLK // SUB, some_rows, 0, unroll=2)


def prepare(step, full, rank, angles, slope, shift):
    dep, rows, cols = full.shape
    plane = lambda n: pltpu.VMEM((n, rows, cols), F32)
    return pl.pallas_call(
        lambda *refs: prepare_kernel(step, *refs),
        out_shape=(
            plane(dep), plane(dep), plane(dep), plane(3 * dep), pltpu.VMEM((rows, cols), F32),
            pltpu.VMEM((3, SUB, cols), F32), plane(dep),
        ),
        in_specs=[VMEM] + [SMEM] * 4,
        out_specs=(VMEM,) * 7,
        scratch_shapes=[
            pltpu.VMEM((2, rows + 2 * PAD, 2 * cols), BF16),
            pltpu.VMEM((2, BLK, 2 * cols), F32),
        ],
        cost_estimate=pl.CostEstimate(flops=10**9, bytes_accessed=10**6, transcendentals=0),
        compiler_params=GRANT,
        name="prepare",
    )(near(full), *(far(x) for x in (rank, angles, slope, shift)))


def mend_kernel(lit_ref, size_ref, gx_ref, flag_ref, x1_ref, x2_ref, lit_out, size_out):
    dep, rows, cols = lit_ref.shape
    even_x = lax.rem(lax.axis_index("tile"), 2) == 0
    k, c = iota2((16, cols))
    spot = jnp.where(k < 8, k % 2 - 2, cols + k % 2)
    x1, x2 = x1_ref[...].astype(F32), x2_ref[...].astype(F32)
    columns = jnp.concatenate([jnp.where(even_x, x2, x1), jnp.where(even_x, x1, x2)], 0)
    columns = columns.T.astype(BF16)
    light_x = flag_ref[2, 0:1, :]
    for z in range(dep):
        beside = jnp.where((k % 8) // 2 == z, stencil(spot - c), 0.0).astype(BF16)
        for b in range(rows // BLK):
            row = slice(b * BLK, (b + 1) * BLK)
            more = dot(columns[row], beside)
            lit_out[z, row, :] = lit_ref[z, row, :] + light_x * more
            size_out[z, row, :] = size_ref[z, row, :] + more * (2.0 * gx_ref[z, row, :] + more)


def mend(lit, size, gx, flag, x1, x2):
    return pl.pallas_call(
        mend_kernel,
        out_shape=(pltpu.VMEM(lit.shape, F32), pltpu.VMEM(size.shape, F32)),
        in_specs=[VMEM] * 6,
        out_specs=(VMEM, VMEM),
        input_output_aliases={0: 0, 1: 1},
        cost_estimate=pl.CostEstimate(flops=10**8, bytes_accessed=10**6, transcendentals=0),
        compiler_params=GRANT,
        name="mend",
    )(*(near(x) for x in (lit, size, gx, flag, x1, x2)))


def shade_kernel(
    z1_ref, z2_ref, lit_ref, size_ref, part_ref, coef_ref, cover_ref, flag_ref,
    image_ref, mean_ref,
):
    cols = lit_ref.shape[2]
    even_z = lax.rem(lax.axis_index("depth"), 2) == 1
    light_z = flag_ref[0, 0:8, :]

    def group(i, carry, start=0, z1_ref=z1_ref):
        r = start + i
        row = pl.ds(pl.multiple_of(8 * r, 8), 8)
        one, two = z1_ref[i].astype(F32), z2_ref[r].astype(F32)
        low = jnp.where(even_z, two, one)
        high = jnp.where(even_z, one, two)
        part = [part_ref[z, row, :] for z in range(4)]
        gz = (
            part[0] + (low[0:8] - 8.0 * low[8:16]),
            part[1] + low[8:16],
            part[2] - high[0:8],
            part[3] + (8.0 * high[0:8] - high[8:16]),
        )
        shade = []
        for z in range(4):
            lit = lit_ref[z, row, :] + light_z * gz[z]
            size = size_ref[z, row, :] + gz[z] * gz[z]
            shade.append(0.25 + 0.75 * (jnp.abs(lit) * lax.rsqrt(size)))
        out = []
        for n in range(3):
            p = [shade[z] * coef_ref[3 * z + n, row, :] for z in range(4)]
            out.append(encode((p[0] + p[1]) + (p[2] + p[3])))
        out.append(cover_ref[row, :])
        image_ref[seat(r)] = jnp.concatenate(out, 0).astype(BF16)
        mean_ref[0, row, :] = 0.25 * ((shade[0] + shade[1]) + (shade[2] + shade[3]))
        return carry

    start = 0
    for ref in (z1_ref,):
        body = functools.partial(group, start=start, z1_ref=ref)
        lax.fori_loop(0, ref.shape[0], body, 0, unroll=8)
        start += ref.shape[0]


def shade(z1, z2, ready):
    _, rows, cols = ready[0].shape
    return pl.pallas_call(
        shade_kernel,
        out_shape=(
            pltpu.VMEM((rows // 8, 32, cols), BF16),
            pltpu.VMEM((1, rows, cols), F32),
        ),
        in_specs=[VMEM] * 8,
        out_specs=(VMEM, VMEM),
        compiler_params=GRANT,
        name="shade",
    )(*(near(x) for x in (z1, z2, *ready)))


def compose_kernel(part_ref, flag_ref, mean_ref, image_ref, out_ref, sem):
    copy = pltpu.make_async_copy(mean_ref, out_ref, sem)
    copy.start()
    slabs, _, cols = part_ref.shape
    ascending = jnp.max(flag_ref[1, 0:8, :]) > 0.5

    def body(i, carry):
        through, red, green, blue = carry
        tile = decode(part_ref[seat(jnp.where(ascending, i, slabs - 1 - i))].astype(F32))
        red = red + through * tile[0:8]
        green = green + through * tile[8:16]
        blue = blue + through * tile[16:24]
        return (through * (1.0 - tile[24:32]), red, green, blue)

    zero = jnp.zeros((8, cols), F32)
    through, red, green, blue = lax.fori_loop(
        0, slabs, body, (jnp.ones((8, cols), F32), zero, zero, zero), unroll=8
    )
    image_ref[0] = red
    image_ref[1] = green
    image_ref[2] = blue
    image_ref[3] = 1.0 - through
    copy.wait()


def compose(parts, flag, mean):
    return pl.pallas_call(
        compose_kernel,
        out_shape=(
            jax.ShapeDtypeStruct((4, 8, parts.shape[2]), F32),
            jax.ShapeDtypeStruct(mean.shape, F32),
        ),
        in_specs=[VMEM] * 3,
        out_specs=(VMEM, pl.BlockSpec(memory_space=pltpu.HBM)),
        scratch_shapes=[pltpu.SemaphoreType.DMA],
        compiler_params=GRANT,
        name="compose",
    )(near(parts), near(flag), near(mean))


def mates(count, start):
    low = range(start, count - 1, 2)
    return [(i, i + 1) for i in low] + [(i + 1, i) for i in low]


def shards(coarse, residual, levels, slab_rank, light_angles, color_slope, color_shift):
    dep = residual.shape[0]
    slabs, tiles = lax.axis_size("depth"), lax.axis_size("tile")
    step = 4.0 / (dep * slabs)
    full, z1, z2, x1, x2 = refine(residual, coarse, levels)
    z1 = lax.ppermute(z1, "depth", mates(slabs, 1))
    z2 = lax.ppermute(z2, "depth", mates(slabs, 0))
    x1 = lax.ppermute(x1, "tile", mates(tiles, 0))
    x2 = lax.ppermute(x2, "tile", mates(tiles, 1))
    *ready, gx = prepare(step, full, slab_rank, light_angles, color_slope, color_shift)
    ready[:2] = mend(*ready[:2], gx, ready[-1], x1, x2)
    image, mean = shade(z1, z2, ready)
    order = sorted(range(slabs), key=seat)
    parts = lax.all_to_all(
        image, "depth", split_axis=0, concat_axis=0, tiled=True, axis_index_groups=[order]
    )
    return compose(parts, ready[-1], mean)


def solution(mesh):
    placed = (
        P("depth", None, "tile"),
        P("depth", None, "tile"),
        P("depth", None, "tile"),
        P(),
        P(),
        P(),
        P(),
    )
    return jax.shard_map(
        shards,
        mesh=mesh,
        in_specs=placed,
        out_specs=(P(None, "depth", "tile"), P("depth", None, "tile")),
        check_vma=False,
    )
```

```python
import functools

import jax
import jax.numpy as jnp
from jax import lax
from jax.experimental import pallas as pl
from jax.experimental.pallas import tpu as pltpu
from jax.sharding import PartitionSpec as P

F32 = jnp.float32
BF16 = jnp.bfloat16
VMEM = pl.BlockSpec(memory_space=pltpu.VMEM)
SMEM = pl.BlockSpec(memory_space=pltpu.SMEM)
NN = (((1,), (0,)), ((), ()))
NT = (((1,), (1,)), ((), ()))
PAD = 64
BLK = 128
SUB = 16


GRANT = pltpu.CompilerParams(vmem_limit_bytes=12 * 2**20)
GAIN = 16.0


def far(x):
    return pltpu.with_memory_space_constraint(x, pltpu.HBM)


def near(x):
    return pltpu.with_memory_space_constraint(x, pltpu.VMEM)


def dot(a, b, dims=NN):
    return lax.dot_general(a, b, dims, preferred_element_type=F32)


def iota2(shape):
    return (
        lax.broadcasted_iota(jnp.int32, shape, 0),
        lax.broadcasted_iota(jnp.int32, shape, 1),
    )


def repeater(out, inner):
    r, c = iota2((out, inner))
    return jnp.where(r // (out // inner) == c, 1.0, 0.0).astype(BF16)


def stencil(offset):
    w = jnp.where(offset == -2, 1.0, jnp.where(offset == -1, -8.0, 0.0))
    return jnp.where(offset == 1, 8.0, jnp.where(offset == 2, -1.0, w))


def seat(d):
    y, x, z = d >> 4, (d >> 2) & 3, d & 3
    return (3 - z) * 16 + (3 - y) * 4 + (3 - x)


def encode(x):
    x = x * GAIN
    x = x * x
    return x * x


def decode(x):
    for _ in range(2):
        x = x * lax.rsqrt(jnp.maximum(x, 1e-37))
    return x * (1.0 / GAIN)


def refine_kernel(
    res_ref, coarse_ref, level_ref, full_ref, z1_ref, z2_ref
):
    dep, rows, cols = res_ref.shape
    half = coarse_ref.shape[2]
    even_z = lax.rem(lax.axis_index("depth"), 2) == 1
    widen2 = repeater(cols, coarse_ref.shape[1])
    widen4 = repeater(cols, level_ref.shape[0])
    lev = dot(widen4, level_ref[...].astype(F32).astype(BF16)).astype(BF16)
    scale = 0.5 * dot(repeater(rows, lev.shape[1]), lev, NT)
    tall2 = repeater(256, 128)
    wide = [dot(widen2, coarse_ref[zc]).astype(BF16) for zc in range(dep // 2)]
    for b in range(half // 128):
        part = pl.ds(b * 256, 256)
        packs = []
        for zc in range(dep // 2):
            lifted = dot(tall2, wide[zc][:, b * 128 : (b + 1) * 128], NT)
            both = [
                lifted + scale[b * 256 : (b + 1) * 256] * res_ref[z, part, :].astype(F32)
                for z in (2 * zc, 2 * zc + 1)
            ]
            for q in range(2):
                full_ref[2 * zc + q, part, :] = both[q].astype(BF16)
            packs.append(
                jnp.concatenate([v.reshape(32, 8, cols) for v in both], 1).astype(BF16)
            )
        group = pl.ds(b * 32, 32)
        z1_ref[group] = jnp.where(even_z, packs[1], packs[0])
        z2_ref[group] = jnp.where(even_z, packs[0], packs[1])


def columns_kernel(full_ref, x1_ref, x2_ref):
    dep, rows, cols = full_ref.shape
    even_x = lax.rem(lax.axis_index("tile"), 2) == 0
    k, c = iota2((16, cols))
    edges = jnp.zeros((16, rows), F32)
    for z in range(dep):
        col = jnp.where(k < 8, k - 2 * z + cols - 2, k - 8 - 2 * z)
        mine = (k % 8) // 2 == z
        pick = jnp.where(mine & (col == c), 1.0, 0.0).astype(BF16)
        edges = edges + dot(pick, full_ref[z], NT)
    last, first = edges[0:8], edges[8:16]
    x1_ref[...] = jnp.where(even_x, last, first).astype(BF16)
    x2_ref[...] = jnp.where(even_x, first, last).astype(BF16)


def columns(full):
    dep, rows, _ = full.shape
    edge = pltpu.VMEM((2 * dep, rows), BF16)
    return pl.pallas_call(
        columns_kernel,
        out_shape=(edge, edge),
        in_specs=[VMEM],
        out_specs=(VMEM, VMEM),
        cost_estimate=pl.CostEstimate(flops=10**8, bytes_accessed=10**6, transcendentals=0),
        compiler_params=GRANT,
        name="columns",
    )(near(full))


def refine(residual, coarse, levels):
    dep, rows, cols = residual.shape
    plane = pltpu.VMEM((rows // 8, 16, cols), BF16)
    return pl.pallas_call(
        refine_kernel,
        out_shape=(pltpu.VMEM((dep, rows, cols), BF16), plane, plane),
        in_specs=[VMEM] * 3,
        out_specs=(VMEM,) * 3,
        cost_estimate=pl.CostEstimate(flops=10**8, bytes_accessed=10**6, transcendentals=0),
        compiler_params=GRANT,
        name="refine",
    )(*(far(x) for x in (residual, jnp.swapaxes(coarse, 1, 2), jnp.swapaxes(levels[0], 0, 1))))


def prepare_kernel(
    step, full_ref, rank_ref, angle_ref, slope_ref, shift_ref,
    lit_ref, size_ref, part_ref, coef_ref, cover_ref, flag_ref, gx_ref, pair, gy_ref,
):
    dep, rows, cols = full_ref.shape
    slabs = rank_ref.shape[0]
    ascending = rank_ref[0] < rank_ref[slabs - 1]
    visible = jnp.where(rank_ref[lax.axis_index("depth")] >= 0, 1.0, 0.0).astype(F32)
    azimuth = jnp.full((SUB, cols), angle_ref[0], F32)
    elevation = jnp.full((SUB, cols), angle_ref[1], F32)
    light_y = jnp.cos(elevation) * jnp.sin(azimuth)
    light_x = jnp.cos(elevation) * jnp.cos(azimuth)
    slope = [0.5 * slope_ref[k] for k in range(3)]
    shift = [0.5 * shift_ref[k] for k in range(3)]
    flag_ref[0] = jnp.sin(elevation)
    flag_ref[1] = jnp.full((SUB, cols), jnp.where(ascending, 1.0, 0.0), F32)
    flag_ref[2] = light_x

    zero = jnp.zeros((PAD, 2 * cols), BF16)
    for p in range(2):
        pair[p, 0:PAD, :] = zero
        pair[p, PAD + rows :, :] = zero
        for q in range(2):
            pair[p, PAD : PAD + rows, q * cols : (q + 1) * cols] = full_ref[2 * p + q]

    r, c = iota2((cols, cols))
    across = stencil(r - c).astype(BF16)
    r, c = iota2((BLK, BLK + 2 * PAD))
    along = stencil(c - PAD - r).astype(BF16)
    for b in range(rows // BLK):
        base = b * BLK
        for p in range(2):
            gy_ref[p] = dot(along, pair[p, base : base + BLK + 2 * PAD, :])
            for q in range(2):
                z = 2 * p + q
                gx_ref[z, base : base + BLK, :] = dot(full_ref[z, base : base + BLK, :], across)

        def some_rows(i, carry, base=base):
            at = pl.ds(pl.multiple_of(i * SUB, SUB), SUB)
            row = pl.ds(pl.multiple_of(base + i * SUB, SUB), SUB)
            own = [full_ref[z, row, :].astype(F32) for z in range(4)]
            part_ref[0, row, :] = 8.0 * own[1] - own[2]
            part_ref[1, row, :] = 8.0 * (own[2] - own[0]) - own[3]
            part_ref[2, row, :] = 8.0 * (own[3] - own[1]) + own[0]
            part_ref[3, row, :] = own[1] - 8.0 * own[2]
            clear, color = [], []
            for z in range(4):
                v = own[z]
                gy = gy_ref[z // 2, at, (z % 2) * cols : (z % 2 + 1) * cols]
                gx = gx_ref[z, row, :]
                lit_ref[z, row, :] = light_y * gy + light_x * gx
                size_ref[z, row, :] = gy * gy + gx * gx + 144.0
                extinct = 2.0 + 2.0 * jnp.tanh(1.5 * v - 2.25)
                clear.append(jnp.exp(-step * extinct))
                color.append([0.5 + 0.5 * jnp.tanh(slope[n] * v + shift[n]) for n in range(3)])
            up = [None, clear[0], clear[0] * clear[1], None]
            up[3] = up[2] * clear[2]
            down = [None, None, clear[3], None]
            down[1] = clear[3] * clear[2]
            down[0] = down[1] * clear[1]
            before = [
                jnp.where(ascending, 1.0, down[0]),
                jnp.where(ascending, up[1], down[1]),
                jnp.where(ascending, up[2], down[2]),
                jnp.where(ascending, up[3], 1.0),
            ]
            for z in range(4):
                weight = before[z] * (1.0 - clear[z]) * visible
                for n in range(3):
                    coef_ref[3 * z + n, row, :] = weight * color[z][n]
            cover_ref[row, :] = encode((1.0 - up[3] * clear[3]) * visible)
            return carry

        lax.fori_loop(0, BLK // SUB, some_rows, 0, unroll=2)


def prepare(step, full, rank, angles, slope, shift):
    dep, rows, cols = full.shape
    plane = lambda n: pltpu.VMEM((n, rows, cols), F32)
    return pl.pallas_call(
        lambda *refs: prepare_kernel(step, *refs),
        out_shape=(
            plane(dep), plane(dep), plane(dep), plane(3 * dep), pltpu.VMEM((rows, cols), F32),
            pltpu.VMEM((3, SUB, cols), F32), plane(dep),
        ),
        in_specs=[VMEM] + [SMEM] * 4,
        out_specs=(VMEM,) * 7,
        scratch_shapes=[
            pltpu.VMEM((2, rows + 2 * PAD, 2 * cols), BF16),
            pltpu.VMEM((2, BLK, 2 * cols), F32),
        ],
        cost_estimate=pl.CostEstimate(flops=10**9, bytes_accessed=10**6, transcendentals=0),
        compiler_params=GRANT,
        name="prepare",
    )(near(full), *(far(x) for x in (rank, angles, slope, shift)))


def mend_kernel(lit_ref, size_ref, gx_ref, flag_ref, x1_ref, x2_ref, lit_out, size_out):
    dep, rows, cols = lit_ref.shape
    even_x = lax.rem(lax.axis_index("tile"), 2) == 0
    k, c = iota2((16, cols))
    spot = jnp.where(k < 8, k % 2 - 2, cols + k % 2)
    x1, x2 = x1_ref[...].astype(F32), x2_ref[...].astype(F32)
    columns = jnp.concatenate([jnp.where(even_x, x2, x1), jnp.where(even_x, x1, x2)], 0)
    columns = columns.T.astype(BF16)
    light_x = flag_ref[2, 0:1, :]
    for z in range(dep):
        beside = jnp.where((k % 8) // 2 == z, stencil(spot - c), 0.0).astype(BF16)
        for b in range(rows // BLK):
            row = slice(b * BLK, (b + 1) * BLK)
            more = dot(columns[row], beside)
            lit_out[z, row, :] = lit_ref[z, row, :] + light_x * more
            size_out[z, row, :] = size_ref[z, row, :] + more * (2.0 * gx_ref[z, row, :] + more)


def mend(lit, size, gx, flag, x1, x2):
    return pl.pallas_call(
        mend_kernel,
        out_shape=(pltpu.VMEM(lit.shape, F32), pltpu.VMEM(size.shape, F32)),
        in_specs=[VMEM] * 6,
        out_specs=(VMEM, VMEM),
        input_output_aliases={0: 0, 1: 1},
        cost_estimate=pl.CostEstimate(flops=10**8, bytes_accessed=10**6, transcendentals=0),
        compiler_params=GRANT,
        name="mend",
    )(*(near(x) for x in (lit, size, gx, flag, x1, x2)))


def shade_kernel(
    z1_ref, z2_ref, lit_ref, size_ref, part_ref, coef_ref, cover_ref, flag_ref,
    image_ref, mean_ref,
):
    cols = lit_ref.shape[2]
    even_z = lax.rem(lax.axis_index("depth"), 2) == 1
    light_z = flag_ref[0, 0:8, :]

    def group(i, carry, start=0, z1_ref=z1_ref):
        r = start + i
        row = pl.ds(pl.multiple_of(8 * r, 8), 8)
        one, two = z1_ref[i].astype(F32), z2_ref[r].astype(F32)
        low = jnp.where(even_z, two, one)
        high = jnp.where(even_z, one, two)
        part = [part_ref[z, row, :] for z in range(4)]
        gz = (
            part[0] + (low[0:8] - 8.0 * low[8:16]),
            part[1] + low[8:16],
            part[2] - high[0:8],
            part[3] + (8.0 * high[0:8] - high[8:16]),
        )
        shade = []
        for z in range(4):
            lit = lit_ref[z, row, :] + light_z * gz[z]
            size = size_ref[z, row, :] + gz[z] * gz[z]
            shade.append(0.25 + 0.75 * (jnp.abs(lit) * lax.rsqrt(size)))
        out = []
        for n in range(3):
            p = [shade[z] * coef_ref[3 * z + n, row, :] for z in range(4)]
            out.append(encode((p[0] + p[1]) + (p[2] + p[3])))
        out.append(cover_ref[row, :])
        image_ref[seat(r)] = jnp.concatenate(out, 0).astype(BF16)
        mean_ref[0, row, :] = 0.25 * ((shade[0] + shade[1]) + (shade[2] + shade[3]))
        return carry

    start = 0
    for ref in (z1_ref,):
        body = functools.partial(group, start=start, z1_ref=ref)
        lax.fori_loop(0, ref.shape[0], body, 0, unroll=8)
        start += ref.shape[0]


def shade(z1, z2, ready):
    _, rows, cols = ready[0].shape
    return pl.pallas_call(
        shade_kernel,
        out_shape=(
            pltpu.VMEM((rows // 8, 32, cols), BF16),
            pltpu.VMEM((1, rows, cols), F32),
        ),
        in_specs=[VMEM] * 8,
        out_specs=(VMEM, VMEM),
        compiler_params=GRANT,
        name="shade",
    )(*(near(x) for x in (z1, z2, *ready)))


def compose_kernel(part_ref, flag_ref, mean_ref, image_ref, out_ref, sem):
    copy = pltpu.make_async_copy(mean_ref, out_ref, sem)
    copy.start()
    slabs, _, cols = part_ref.shape
    ascending = jnp.max(flag_ref[1, 0:8, :]) > 0.5

    def body(i, carry):
        through, red, green, blue = carry
        tile = decode(part_ref[seat(jnp.where(ascending, i, slabs - 1 - i))].astype(F32))
        red = red + through * tile[0:8]
        green = green + through * tile[8:16]
        blue = blue + through * tile[16:24]
        return (through * (1.0 - tile[24:32]), red, green, blue)

    zero = jnp.zeros((8, cols), F32)
    through, red, green, blue = lax.fori_loop(
        0, slabs, body, (jnp.ones((8, cols), F32), zero, zero, zero), unroll=8
    )
    image_ref[0] = red
    image_ref[1] = green
    image_ref[2] = blue
    image_ref[3] = 1.0 - through
    copy.wait()


def compose(parts, flag, mean):
    return pl.pallas_call(
        compose_kernel,
        out_shape=(
            jax.ShapeDtypeStruct((4, 8, parts.shape[2]), F32),
            jax.ShapeDtypeStruct(mean.shape, F32),
        ),
        in_specs=[VMEM] * 3,
        out_specs=(VMEM, pl.BlockSpec(memory_space=pltpu.HBM)),
        scratch_shapes=[pltpu.SemaphoreType.DMA],
        compiler_params=GRANT,
        name="compose",
    )(near(parts), near(flag), near(mean))


def mates(count, start):
    low = range(start, count - 1, 2)
    return [(i, i + 1) for i in low] + [(i + 1, i) for i in low]


def shards(coarse, residual, levels, slab_rank, light_angles, color_slope, color_shift):
    dep = residual.shape[0]
    slabs, tiles = lax.axis_size("depth"), lax.axis_size("tile")
    step = 4.0 / (dep * slabs)
    full, z1, z2 = refine(residual, coarse, levels)
    x1, x2 = columns(full)
    z1 = lax.ppermute(z1, "depth", mates(slabs, 1))
    z2 = lax.ppermute(z2, "depth", mates(slabs, 0))
    x1 = lax.ppermute(x1, "tile", mates(tiles, 0))
    x2 = lax.ppermute(x2, "tile", mates(tiles, 1))
    *ready, gx = prepare(step, full, slab_rank, light_angles, color_slope, color_shift)
    ready[:2] = mend(*ready[:2], gx, ready[-1], x1, x2)
    image, mean = shade(z1, z2, ready)
    order = sorted(range(slabs), key=seat)
    parts = lax.all_to_all(
        image, "depth", split_axis=0, concat_axis=0, tiled=True, axis_index_groups=[order]
    )
    return compose(parts, ready[-1], mean)


def solution(mesh):
    placed = (
        P("depth", None, "tile"),
        P("depth", None, "tile"),
        P("depth", None, "tile"),
        P(),
        P(),
        P(),
        P(),
    )
    return jax.shard_map(
        shards,
        mesh=mesh,
        in_specs=placed,
        out_specs=(P(None, "depth", "tile"), P("depth", None, "tile")),
        check_vma=False,
    )
```

```python
import functools

import jax
import jax.numpy as jnp
from jax import lax
from jax.experimental import pallas as pl
from jax.experimental.pallas import tpu as pltpu
from jax.sharding import PartitionSpec as P

F32 = jnp.float32
BF16 = jnp.bfloat16
VMEM = pl.BlockSpec(memory_space=pltpu.VMEM)
SMEM = pl.BlockSpec(memory_space=pltpu.SMEM)
NN = (((1,), (0,)), ((), ()))
NT = (((1,), (1,)), ((), ()))
PAD = 64
BLK = 128
SUB = 16


GRANT = pltpu.CompilerParams(vmem_limit_bytes=12 * 2**20)
GAIN = 16.0


def far(x):
    return pltpu.with_memory_space_constraint(x, pltpu.HBM)


def near(x):
    return pltpu.with_memory_space_constraint(x, pltpu.VMEM)


def dot(a, b, dims=NN):
    return lax.dot_general(a, b, dims, preferred_element_type=F32)


def iota2(shape):
    return (
        lax.broadcasted_iota(jnp.int32, shape, 0),
        lax.broadcasted_iota(jnp.int32, shape, 1),
    )


def repeater(out, inner):
    r, c = iota2((out, inner))
    return jnp.where(r // (out // inner) == c, 1.0, 0.0).astype(BF16)


def stencil(offset):
    w = jnp.where(offset == -2, 1.0, jnp.where(offset == -1, -8.0, 0.0))
    return jnp.where(offset == 1, 8.0, jnp.where(offset == 2, -1.0, w))


def seat(d):
    y, x, z = d >> 4, (d >> 2) & 3, d & 3
    return (3 - z) * 16 + (3 - y) * 4 + (3 - x)


def encode(x):
    x = x * GAIN
    x = x * x
    return x * x


def decode(x):
    for _ in range(2):
        x = x * lax.rsqrt(jnp.maximum(x, 1e-37))
    return x * (1.0 / GAIN)


def refine_kernel(
    res_ref, coarse_ref, level_ref, full_ref, z1_ref, z2_ref
):
    dep, rows, cols = res_ref.shape
    half = coarse_ref.shape[2]
    even_z = lax.rem(lax.axis_index("depth"), 2) == 1
    widen2 = repeater(cols, coarse_ref.shape[1])
    widen4 = repeater(cols, level_ref.shape[0])
    lev = dot(widen4, level_ref[...].astype(F32).astype(BF16)).astype(BF16)
    scale = 0.5 * dot(repeater(rows, lev.shape[1]), lev, NT)
    tall2 = repeater(256, 128)
    wide = [dot(widen2, coarse_ref[zc]).astype(BF16) for zc in range(dep // 2)]
    for b in range(half // 128):
        part = pl.ds(b * 256, 256)
        packs = []
        for zc in range(dep // 2):
            lifted = dot(tall2, wide[zc][:, b * 128 : (b + 1) * 128], NT)
            both = [
                lifted + scale[b * 256 : (b + 1) * 256] * res_ref[z, part, :].astype(F32)
                for z in (2 * zc, 2 * zc + 1)
            ]
            for q in range(2):
                full_ref[2 * zc + q, part, :] = both[q].astype(BF16)
            packs.append(
                jnp.concatenate([v.reshape(32, 8, cols) for v in both], 1).astype(BF16)
            )
        group = pl.ds(b * 32, 32)
        z1_ref[group] = jnp.where(even_z, packs[1], packs[0])
        z2_ref[group] = jnp.where(even_z, packs[0], packs[1])


def columns_kernel(full_ref, x1_ref, x2_ref):
    dep, rows, cols = full_ref.shape
    even_x = lax.rem(lax.axis_index("tile"), 2) == 0
    k, c = iota2((16, cols))
    edges = jnp.zeros((16, rows), F32)
    for z in range(dep):
        col = jnp.where(k < 8, k - 2 * z + cols - 2, k - 8 - 2 * z)
        mine = (k % 8) // 2 == z
        pick = jnp.where(mine & (col == c), 1.0, 0.0).astype(BF16)
        edges = edges + dot(pick, full_ref[z], NT)
    last, first = edges[0:8], edges[8:16]
    x1_ref[...] = jnp.where(even_x, last, first).astype(BF16)
    x2_ref[...] = jnp.where(even_x, first, last).astype(BF16)


def columns(full):
    dep, rows, _ = full.shape
    edge = pltpu.VMEM((2 * dep, rows), BF16)
    return pl.pallas_call(
        columns_kernel,
        out_shape=(edge, edge),
        in_specs=[VMEM],
        out_specs=(VMEM, VMEM),
        cost_estimate=pl.CostEstimate(flops=10**8, bytes_accessed=10**6, transcendentals=0),
        compiler_params=GRANT,
        name="columns",
    )(near(full))


def refine(residual, coarse, levels):
    dep, rows, cols = residual.shape
    plane = pltpu.VMEM((rows // 8, 16, cols), BF16)
    return pl.pallas_call(
        refine_kernel,
        out_shape=(pltpu.VMEM((dep, rows, cols), BF16), plane, plane),
        in_specs=[VMEM] * 3,
        out_specs=(VMEM,) * 3,
        cost_estimate=pl.CostEstimate(flops=10**8, bytes_accessed=10**6, transcendentals=0),
        compiler_params=GRANT,
        name="refine",
    )(*(far(x) for x in (residual, jnp.swapaxes(coarse, 1, 2), jnp.swapaxes(levels[0], 0, 1))))


def prepare_kernel(
    step, full_ref, rank_ref, angle_ref, slope_ref, shift_ref,
    lit_ref, size_ref, part_ref, coef_ref, cover_ref, flag_ref, gx_ref, order_ref, pair, gy_ref,
):
    dep, rows, cols = full_ref.shape
    slabs = rank_ref.shape[0]
    ascending = rank_ref[0] < rank_ref[slabs - 1]
    visible = jnp.where(rank_ref[lax.axis_index("depth")] >= 0, 1.0, 0.0).astype(F32)
    azimuth = jnp.full((SUB, cols), angle_ref[0], F32)
    elevation = jnp.full((SUB, cols), angle_ref[1], F32)
    light_y = jnp.cos(elevation) * jnp.sin(azimuth)
    light_x = jnp.cos(elevation) * jnp.cos(azimuth)
    slope = [0.5 * slope_ref[k] for k in range(3)]
    shift = [0.5 * shift_ref[k] for k in range(3)]
    flag_ref[0] = jnp.sin(elevation)
    flag_ref[1] = jnp.full((SUB, cols), jnp.where(ascending, 1.0, 0.0), F32)
    flag_ref[2] = light_x
    order_ref[0] = jnp.where(ascending, 1, 0)

    zero = jnp.zeros((PAD, 2 * cols), BF16)
    for p in range(2):
        pair[p, 0:PAD, :] = zero
        pair[p, PAD + rows :, :] = zero
        for q in range(2):
            pair[p, PAD : PAD + rows, q * cols : (q + 1) * cols] = full_ref[2 * p + q]

    r, c = iota2((cols, cols))
    across = stencil(r - c).astype(BF16)
    r, c = iota2((BLK, BLK + 2 * PAD))
    along = stencil(c - PAD - r).astype(BF16)
    for b in range(rows // BLK):
        base = b * BLK
        for p in range(2):
            gy_ref[p] = dot(along, pair[p, base : base + BLK + 2 * PAD, :])
            for q in range(2):
                z = 2 * p + q
                gx_ref[z, base : base + BLK, :] = dot(full_ref[z, base : base + BLK, :], across)

        def some_rows(i, carry, base=base):
            at = pl.ds(pl.multiple_of(i * SUB, SUB), SUB)
            row = pl.ds(pl.multiple_of(base + i * SUB, SUB), SUB)
            own = [full_ref[z, row, :].astype(F32) for z in range(4)]
            part_ref[0, row, :] = 8.0 * own[1] - own[2]
            part_ref[1, row, :] = 8.0 * (own[2] - own[0]) - own[3]
            part_ref[2, row, :] = 8.0 * (own[3] - own[1]) + own[0]
            part_ref[3, row, :] = own[1] - 8.0 * own[2]
            clear, color = [], []
            for z in range(4):
                v = own[z]
                gy = gy_ref[z // 2, at, (z % 2) * cols : (z % 2 + 1) * cols]
                gx = gx_ref[z, row, :]
                lit_ref[z, row, :] = light_y * gy + light_x * gx
                size_ref[z, row, :] = gy * gy + gx * gx + 144.0
                extinct = 2.0 + 2.0 * jnp.tanh(1.5 * v - 2.25)
                clear.append(jnp.exp(-step * extinct))
                color.append([0.5 + 0.5 * jnp.tanh(slope[n] * v + shift[n]) for n in range(3)])
            up = [None, clear[0], clear[0] * clear[1], None]
            up[3] = up[2] * clear[2]
            down = [None, None, clear[3], None]
            down[1] = clear[3] * clear[2]
            down[0] = down[1] * clear[1]
            before = [
                jnp.where(ascending, 1.0, down[0]),
                jnp.where(ascending, up[1], down[1]),
                jnp.where(ascending, up[2], down[2]),
                jnp.where(ascending, up[3], 1.0),
            ]
            for z in range(4):
                weight = before[z] * (1.0 - clear[z]) * visible
                for n in range(3):
                    coef_ref[3 * z + n, row, :] = weight * color[z][n]
            cover_ref[row, :] = encode((1.0 - up[3] * clear[3]) * visible)
            return carry

        lax.fori_loop(0, BLK // SUB, some_rows, 0, unroll=2)


def prepare(step, full, rank, angles, slope, shift):
    dep, rows, cols = full.shape
    plane = lambda n: pltpu.VMEM((n, rows, cols), F32)
    return pl.pallas_call(
        lambda *refs: prepare_kernel(step, *refs),
        out_shape=(
            plane(dep), plane(dep), plane(dep), plane(3 * dep), pltpu.VMEM((rows, cols), F32),
            pltpu.VMEM((3, SUB, cols), F32), plane(dep), pltpu.SMEM((1,), jnp.int32),
        ),
        in_specs=[VMEM] + [SMEM] * 4,
        out_specs=(VMEM,) * 7 + (SMEM,),
        scratch_shapes=[
            pltpu.VMEM((2, rows + 2 * PAD, 2 * cols), BF16),
            pltpu.VMEM((2, BLK, 2 * cols), F32),
        ],
        cost_estimate=pl.CostEstimate(flops=10**9, bytes_accessed=10**6, transcendentals=0),
        compiler_params=GRANT,
        name="prepare",
    )(near(full), *(far(x) for x in (rank, angles, slope, shift)))


def mend_kernel(lit_ref, size_ref, gx_ref, flag_ref, x1_ref, x2_ref, lit_out, size_out):
    dep, rows, cols = lit_ref.shape
    even_x = lax.rem(lax.axis_index("tile"), 2) == 0
    k, c = iota2((16, cols))
    spot = jnp.where(k < 8, k % 2 - 2, cols + k % 2)
    x1, x2 = x1_ref[...].astype(F32), x2_ref[...].astype(F32)
    columns = jnp.concatenate([jnp.where(even_x, x2, x1), jnp.where(even_x, x1, x2)], 0)
    columns = columns.T.astype(BF16)
    light_x = flag_ref[2, 0:1, :]
    for z in range(dep):
        beside = jnp.where((k % 8) // 2 == z, stencil(spot - c), 0.0).astype(BF16)
        for b in range(rows // BLK):
            row = slice(b * BLK, (b + 1) * BLK)
            more = dot(columns[row], beside)
            lit_out[z, row, :] = lit_ref[z, row, :] + light_x * more
            size_out[z, row, :] = size_ref[z, row, :] + more * (2.0 * gx_ref[z, row, :] + more)


def mend(lit, size, gx, flag, x1, x2):
    return pl.pallas_call(
        mend_kernel,
        out_shape=(pltpu.VMEM(lit.shape, F32), pltpu.VMEM(size.shape, F32)),
        in_specs=[VMEM] * 6,
        out_specs=(VMEM, VMEM),
        input_output_aliases={0: 0, 1: 1},
        cost_estimate=pl.CostEstimate(flops=10**8, bytes_accessed=10**6, transcendentals=0),
        compiler_params=GRANT,
        name="mend",
    )(*(near(x) for x in (lit, size, gx, flag, x1, x2)))


def shade_kernel(
    z1_ref, z2_ref, lit_ref, size_ref, part_ref, coef_ref, cover_ref, flag_ref,
    image_ref, mean_ref,
):
    cols = lit_ref.shape[2]
    even_z = lax.rem(lax.axis_index("depth"), 2) == 1
    light_z = flag_ref[0, 0:8, :]

    def group(i, carry, start=0, z1_ref=z1_ref):
        r = start + i
        row = pl.ds(pl.multiple_of(8 * r, 8), 8)
        one, two = z1_ref[i].astype(F32), z2_ref[r].astype(F32)
        low = jnp.where(even_z, two, one)
        high = jnp.where(even_z, one, two)
        part = [part_ref[z, row, :] for z in range(4)]
        gz = (
            part[0] + (low[0:8] - 8.0 * low[8:16]),
            part[1] + low[8:16],
            part[2] - high[0:8],
            part[3] + (8.0 * high[0:8] - high[8:16]),
        )
        shade = []
        for z in range(4):
            lit = lit_ref[z, row, :] + light_z * gz[z]
            size = size_ref[z, row, :] + gz[z] * gz[z]
            shade.append(0.25 + 0.75 * (jnp.abs(lit) * lax.rsqrt(size)))
        out = []
        for n in range(3):
            p = [shade[z] * coef_ref[3 * z + n, row, :] for z in range(4)]
            out.append(encode((p[0] + p[1]) + (p[2] + p[3])))
        out.append(cover_ref[row, :])
        image_ref[seat(r)] = jnp.concatenate(out, 0).astype(BF16)
        mean_ref[0, row, :] = 0.25 * ((shade[0] + shade[1]) + (shade[2] + shade[3]))
        return carry

    start = 0
    for ref in (z1_ref,):
        body = functools.partial(group, start=start, z1_ref=ref)
        lax.fori_loop(0, ref.shape[0], body, 0, unroll=16)
        start += ref.shape[0]


def shade(z1, z2, ready):
    _, rows, cols = ready[0].shape
    return pl.pallas_call(
        shade_kernel,
        out_shape=(
            pltpu.VMEM((rows // 8, 32, cols), BF16),
            pltpu.VMEM((1, rows, cols), F32),
        ),
        in_specs=[VMEM] * 8,
        out_specs=(VMEM, VMEM),
        compiler_params=GRANT,
        name="shade",
    )(*(near(x) for x in (z1, z2, *ready)))


def compose_kernel(part_ref, flag_ref, mean_ref, far_ref, out_ref, image_ref, sems):
    copy = pltpu.make_async_copy(mean_ref, out_ref, sems.at[0])
    copy.start()
    slabs, _, cols = part_ref.shape
    ascending = flag_ref[0] > 0

    def body(i, carry):
        through, red, green, blue = carry
        tile = decode(part_ref[seat(jnp.where(ascending, i, slabs - 1 - i))].astype(F32))
        red = red + through * tile[0:8]
        green = green + through * tile[8:16]
        blue = blue + through * tile[16:24]
        return (through * (1.0 - tile[24:32]), red, green, blue)

    zero = jnp.zeros((8, cols), F32)
    through, red, green, blue = lax.fori_loop(
        0, slabs, body, (jnp.ones((8, cols), F32), zero, zero, zero), unroll=8
    )
    image_ref[0] = red
    image_ref[1] = green
    image_ref[2] = blue
    image_ref[3] = 1.0 - through
    last = pltpu.make_async_copy(image_ref, far_ref, sems.at[1])
    last.start()
    copy.wait()
    last.wait()


def compose(parts, flag, mean):
    return pl.pallas_call(
        compose_kernel,
        out_shape=(
            jax.ShapeDtypeStruct((4, 8, parts.shape[2]), F32),
            jax.ShapeDtypeStruct(mean.shape, F32),
        ),
        in_specs=[VMEM, SMEM, VMEM],
        out_specs=(pl.BlockSpec(memory_space=pltpu.HBM),) * 2,
        scratch_shapes=[
            pltpu.VMEM((4, 8, parts.shape[2]), F32),
            pltpu.SemaphoreType.DMA((2,)),
        ],
        compiler_params=GRANT,
        name="compose",
    )(near(parts), pltpu.with_memory_space_constraint(flag, pltpu.SMEM), near(mean))


def mates(count, start):
    low = range(start, count - 1, 2)
    return [(i, i + 1) for i in low] + [(i + 1, i) for i in low]


def shards(coarse, residual, levels, slab_rank, light_angles, color_slope, color_shift):
    dep = residual.shape[0]
    slabs, tiles = lax.axis_size("depth"), lax.axis_size("tile")
    step = 4.0 / (dep * slabs)
    full, z1, z2 = refine(residual, coarse, levels)
    x1, x2 = columns(full)
    z1 = lax.ppermute(z1, "depth", mates(slabs, 1))
    z2 = lax.ppermute(z2, "depth", mates(slabs, 0))
    x1 = lax.ppermute(x1, "tile", mates(tiles, 0))
    x2 = lax.ppermute(x2, "tile", mates(tiles, 1))
    *ready, gx, forward = prepare(step, full, slab_rank, light_angles, color_slope, color_shift)
    ready[:2] = mend(*ready[:2], gx, ready[-1], x1, x2)
    image, mean = shade(z1, z2, ready)
    order = sorted(range(slabs), key=seat)
    parts = lax.all_to_all(
        image, "depth", split_axis=0, concat_axis=0, tiled=True, axis_index_groups=[order]
    )
    return compose(parts, forward, mean)


def solution(mesh):
    placed = (
        P("depth", None, "tile"),
        P("depth", None, "tile"),
        P("depth", None, "tile"),
        P(),
        P(),
        P(),
        P(),
    )
    return jax.shard_map(
        shards,
        mesh=mesh,
        in_specs=placed,
        out_specs=(P(None, "depth", "tile"), P("depth", None, "tile")),
        check_vma=False,
    )
```

```python
import functools

import jax
import jax.numpy as jnp
from jax import lax
from jax.experimental import pallas as pl
from jax.experimental.pallas import tpu as pltpu
from jax.sharding import PartitionSpec as P

F32 = jnp.float32
BF16 = jnp.bfloat16
VMEM = pl.BlockSpec(memory_space=pltpu.VMEM)
SMEM = pl.BlockSpec(memory_space=pltpu.SMEM)
NN = (((1,), (0,)), ((), ()))
NT = (((1,), (1,)), ((), ()))
PAD = 64
BLK = 128
SUB = 16


GRANT = pltpu.CompilerParams(vmem_limit_bytes=12 * 2**20)
GAIN = 16.0


def far(x):
    return pltpu.with_memory_space_constraint(x, pltpu.HBM)


def near(x):
    return pltpu.with_memory_space_constraint(x, pltpu.VMEM)


def dot(a, b, dims=NN):
    return lax.dot_general(a, b, dims, preferred_element_type=F32)


def iota2(shape):
    return (
        lax.broadcasted_iota(jnp.int32, shape, 0),
        lax.broadcasted_iota(jnp.int32, shape, 1),
    )


def repeater(out, inner):
    r, c = iota2((out, inner))
    return jnp.where(r // (out // inner) == c, 1.0, 0.0).astype(BF16)


def stencil(offset):
    w = jnp.where(offset == -2, 1.0, jnp.where(offset == -1, -8.0, 0.0))
    return jnp.where(offset == 1, 8.0, jnp.where(offset == 2, -1.0, w))


def seat(d):
    y, x, z = d >> 4, (d >> 2) & 3, d & 3
    return (3 - z) * 16 + (3 - y) * 4 + (3 - x)


def encode(x):
    x = x * GAIN
    x = x * x
    return x * x


def decode(x):
    for _ in range(2):
        x = x * lax.rsqrt(jnp.maximum(x, 1e-37))
    return x * (1.0 / GAIN)


def refine_kernel(
    res_ref, coarse_ref, level_ref, full_ref, z1_ref, z2_ref
):
    dep, rows, cols = res_ref.shape
    half = coarse_ref.shape[2]
    even_z = lax.rem(lax.axis_index("depth"), 2) == 1
    widen2 = repeater(cols, coarse_ref.shape[1])
    widen4 = repeater(cols, level_ref.shape[0])
    lev = dot(widen4, level_ref[...].astype(F32).astype(BF16)).astype(BF16)
    scale = 0.5 * dot(repeater(rows, lev.shape[1]), lev, NT)
    tall2 = repeater(256, 128)
    wide = [dot(widen2, coarse_ref[zc]).astype(BF16) for zc in range(dep // 2)]
    for b in range(half // 128):
        part = pl.ds(b * 256, 256)
        packs = []
        for zc in range(dep // 2):
            lifted = dot(tall2, wide[zc][:, b * 128 : (b + 1) * 128], NT)
            both = [
                lifted + scale[b * 256 : (b + 1) * 256] * res_ref[z, part, :].astype(F32)
                for z in (2 * zc, 2 * zc + 1)
            ]
            for q in range(2):
                full_ref[2 * zc + q, part, :] = both[q].astype(BF16)
            packs.append(
                jnp.concatenate([v.reshape(32, 8, cols) for v in both], 1).astype(BF16)
            )
        group = pl.ds(b * 32, 32)
        z1_ref[group] = jnp.where(even_z, packs[1], packs[0])
        z2_ref[group] = jnp.where(even_z, packs[0], packs[1])


def columns_kernel(full_ref, x1_ref, x2_ref):
    dep, rows, cols = full_ref.shape
    even_x = lax.rem(lax.axis_index("tile"), 2) == 0
    k, c = iota2((16, cols))
    edges = jnp.zeros((16, rows), F32)
    for z in range(dep):
        col = jnp.where(k < 8, k - 2 * z + cols - 2, k - 8 - 2 * z)
        mine = (k % 8) // 2 == z
        pick = jnp.where(mine & (col == c), 1.0, 0.0).astype(BF16)
        edges = edges + dot(pick, full_ref[z], NT)
    last, first = edges[0:8], edges[8:16]
    x1_ref[...] = jnp.where(even_x, last, first).astype(BF16)
    x2_ref[...] = jnp.where(even_x, first, last).astype(BF16)


def columns(full):
    dep, rows, _ = full.shape
    edge = pltpu.VMEM((2 * dep, rows), BF16)
    return pl.pallas_call(
        columns_kernel,
        out_shape=(edge, edge),
        in_specs=[VMEM],
        out_specs=(VMEM, VMEM),
        cost_estimate=pl.CostEstimate(flops=10**8, bytes_accessed=10**6, transcendentals=0),
        compiler_params=GRANT,
        name="columns",
    )(near(full))


def refine(residual, coarse, levels):
    dep, rows, cols = residual.shape
    plane = pltpu.VMEM((rows // 8, 16, cols), BF16)
    return pl.pallas_call(
        refine_kernel,
        out_shape=(pltpu.VMEM((dep, rows, cols), BF16), plane, plane),
        in_specs=[VMEM] * 3,
        out_specs=(VMEM,) * 3,
        cost_estimate=pl.CostEstimate(flops=10**8, bytes_accessed=10**6, transcendentals=0),
        compiler_params=GRANT,
        name="refine",
    )(*(far(x) for x in (residual, jnp.swapaxes(coarse, 1, 2), jnp.swapaxes(levels[0], 0, 1))))


def prepare_kernel(
    step, full_ref, rank_ref, angle_ref, slope_ref, shift_ref,
    lit_ref, size_ref, part_ref, coef_ref, cover_ref, flag_ref, gx_ref, order_ref, pair, gy_ref,
):
    dep, rows, cols = full_ref.shape
    slabs = rank_ref.shape[0]
    ascending = rank_ref[0] < rank_ref[slabs - 1]
    visible = jnp.where(rank_ref[lax.axis_index("depth")] >= 0, 1.0, 0.0).astype(F32)
    azimuth = jnp.full((SUB, cols), angle_ref[0], F32)
    elevation = jnp.full((SUB, cols), angle_ref[1], F32)
    light_y = jnp.cos(elevation) * jnp.sin(azimuth)
    light_x = jnp.cos(elevation) * jnp.cos(azimuth)
    slope = [0.5 * slope_ref[k] for k in range(3)]
    shift = [0.5 * shift_ref[k] for k in range(3)]
    flag_ref[0] = jnp.sin(elevation)
    flag_ref[1] = jnp.full((SUB, cols), jnp.where(ascending, 1.0, 0.0), F32)
    flag_ref[2] = light_x
    order_ref[0] = jnp.where(ascending, 1, 0)

    zero = jnp.zeros((PAD, 2 * cols), BF16)
    for p in range(2):
        pair[p, 0:PAD, :] = zero
        pair[p, PAD + rows :, :] = zero
        for q in range(2):
            pair[p, PAD : PAD + rows, q * cols : (q + 1) * cols] = full_ref[2 * p + q]

    r, c = iota2((cols, cols))
    across = stencil(r - c).astype(BF16)
    r, c = iota2((BLK, BLK + 2 * PAD))
    along = stencil(c - PAD - r).astype(BF16)
    for b in range(rows // BLK):
        base = b * BLK
        for p in range(2):
            gy_ref[p] = dot(along, pair[p, base : base + BLK + 2 * PAD, :])
            for q in range(2):
                z = 2 * p + q
                gx_ref[z, base : base + BLK, :] = dot(full_ref[z, base : base + BLK, :], across)

        def some_rows(i, carry, base=base):
            at = pl.ds(pl.multiple_of(i * SUB, SUB), SUB)
            row = pl.ds(pl.multiple_of(base + i * SUB, SUB), SUB)
            own = [full_ref[z, row, :].astype(F32) for z in range(4)]
            part_ref[0, row, :] = 8.0 * own[1] - own[2]
            part_ref[1, row, :] = 8.0 * (own[2] - own[0]) - own[3]
            part_ref[2, row, :] = 8.0 * (own[3] - own[1]) + own[0]
            part_ref[3, row, :] = own[1] - 8.0 * own[2]
            clear, color = [], []
            for z in range(4):
                v = own[z]
                gy = gy_ref[z // 2, at, (z % 2) * cols : (z % 2 + 1) * cols]
                gx = gx_ref[z, row, :]
                lit_ref[z, row, :] = light_y * gy + light_x * gx
                size_ref[z, row, :] = gy * gy + gx * gx + 144.0
                extinct = 2.0 + 2.0 * jnp.tanh(1.5 * v - 2.25)
                clear.append(jnp.exp(-step * extinct))
                color.append([0.5 + 0.5 * jnp.tanh(slope[n] * v + shift[n]) for n in range(3)])
            up = [None, clear[0], clear[0] * clear[1], None]
            up[3] = up[2] * clear[2]
            down = [None, None, clear[3], None]
            down[1] = clear[3] * clear[2]
            down[0] = down[1] * clear[1]
            before = [
                jnp.where(ascending, 1.0, down[0]),
                jnp.where(ascending, up[1], down[1]),
                jnp.where(ascending, up[2], down[2]),
                jnp.where(ascending, up[3], 1.0),
            ]
            for z in range(4):
                weight = before[z] * (1.0 - clear[z]) * (0.75 * visible)
                for n in range(3):
                    coef_ref[3 * z + n, row, :] = weight * color[z][n]
            cover_ref[row, :] = encode((1.0 - up[3] * clear[3]) * visible)
            return carry

        lax.fori_loop(0, BLK // SUB, some_rows, 0, unroll=2)


def prepare(step, full, rank, angles, slope, shift):
    dep, rows, cols = full.shape
    plane = lambda n: pltpu.VMEM((n, rows, cols), F32)
    return pl.pallas_call(
        lambda *refs: prepare_kernel(step, *refs),
        out_shape=(
            plane(dep), plane(dep), plane(dep), plane(3 * dep), pltpu.VMEM((rows, cols), F32),
            pltpu.VMEM((3, SUB, cols), F32), plane(dep), pltpu.SMEM((1,), jnp.int32),
        ),
        in_specs=[VMEM] + [SMEM] * 4,
        out_specs=(VMEM,) * 7 + (SMEM,),
        scratch_shapes=[
            pltpu.VMEM((2, rows + 2 * PAD, 2 * cols), BF16),
            pltpu.VMEM((2, BLK, 2 * cols), F32),
        ],
        cost_estimate=pl.CostEstimate(flops=10**9, bytes_accessed=10**6, transcendentals=0),
        compiler_params=GRANT,
        name="prepare",
    )(near(full), *(far(x) for x in (rank, angles, slope, shift)))


def mend_kernel(lit_ref, size_ref, gx_ref, flag_ref, x1_ref, x2_ref, lit_out, size_out):
    dep, rows, cols = lit_ref.shape
    even_x = lax.rem(lax.axis_index("tile"), 2) == 0
    k, c = iota2((16, cols))
    spot = jnp.where(k < 8, k % 2 - 2, cols + k % 2)
    x1, x2 = x1_ref[...].astype(F32), x2_ref[...].astype(F32)
    columns = jnp.concatenate([jnp.where(even_x, x2, x1), jnp.where(even_x, x1, x2)], 0)
    columns = columns.T.astype(BF16)
    light_x = flag_ref[2, 0:1, :]
    for z in range(dep):
        beside = jnp.where((k % 8) // 2 == z, stencil(spot - c), 0.0).astype(BF16)
        for b in range(rows // BLK):
            row = slice(b * BLK, (b + 1) * BLK)
            more = dot(columns[row], beside)
            lit_out[z, row, :] = lit_ref[z, row, :] + light_x * more
            size_out[z, row, :] = size_ref[z, row, :] + more * (2.0 * gx_ref[z, row, :] + more)


def mend(lit, size, gx, flag, x1, x2):
    return pl.pallas_call(
        mend_kernel,
        out_shape=(pltpu.VMEM(lit.shape, F32), pltpu.VMEM(size.shape, F32)),
        in_specs=[VMEM] * 6,
        out_specs=(VMEM, VMEM),
        input_output_aliases={0: 0, 1: 1},
        cost_estimate=pl.CostEstimate(flops=10**8, bytes_accessed=10**6, transcendentals=0),
        compiler_params=GRANT,
        name="mend",
    )(*(near(x) for x in (lit, size, gx, flag, x1, x2)))


def shade_kernel(
    z1_ref, z2_ref, lit_ref, size_ref, part_ref, coef_ref, cover_ref, flag_ref,
    image_ref, mean_ref,
):
    cols = lit_ref.shape[2]
    even_z = lax.rem(lax.axis_index("depth"), 2) == 1
    light_z = flag_ref[0, 0:8, :]

    def group(i, carry, start=0, z1_ref=z1_ref):
        r = start + i
        row = pl.ds(pl.multiple_of(8 * r, 8), 8)
        one, two = z1_ref[i].astype(F32), z2_ref[r].astype(F32)
        low = jnp.where(even_z, two, one)
        high = jnp.where(even_z, one, two)
        part = [part_ref[z, row, :] for z in range(4)]
        gz = (
            part[0] + (low[0:8] - 8.0 * low[8:16]),
            part[1] + low[8:16],
            part[2] - high[0:8],
            part[3] + (8.0 * high[0:8] - high[8:16]),
        )
        shade = []
        for z in range(4):
            lit = lit_ref[z, row, :] + light_z * gz[z]
            size = size_ref[z, row, :] + gz[z] * gz[z]
            shade.append(jnp.abs(lit) * lax.rsqrt(size) + 1.0 / 3.0)
        out = []
        for n in range(3):
            p = [shade[z] * coef_ref[3 * z + n, row, :] for z in range(4)]
            out.append(encode((p[0] + p[1]) + (p[2] + p[3])))
        out.append(cover_ref[row, :])
        image_ref[seat(r)] = jnp.concatenate(out, 0).astype(BF16)
        mean_ref[0, row, :] = 0.1875 * ((shade[0] + shade[1]) + (shade[2] + shade[3]))
        return carry

    start = 0
    for ref in (z1_ref,):
        body = functools.partial(group, start=start, z1_ref=ref)
        lax.fori_loop(0, ref.shape[0], body, 0, unroll=16)
        start += ref.shape[0]


def shade(z1, z2, ready):
    _, rows, cols = ready[0].shape
    return pl.pallas_call(
        shade_kernel,
        out_shape=(
            pltpu.VMEM((rows // 8, 32, cols), BF16),
            pltpu.VMEM((1, rows, cols), F32),
        ),
        in_specs=[VMEM] * 8,
        out_specs=(VMEM, VMEM),
        compiler_params=GRANT,
        name="shade",
    )(*(near(x) for x in (z1, z2, *ready)))


def compose_kernel(part_ref, flag_ref, mean_ref, far_ref, out_ref, image_ref, sems):
    copy = pltpu.make_async_copy(mean_ref, out_ref, sems.at[0])
    copy.start()
    slabs, _, cols = part_ref.shape
    ascending = flag_ref[0] > 0

    def body(i, carry):
        through, red, green, blue = carry
        tile = decode(part_ref[seat(jnp.where(ascending, i, slabs - 1 - i))].astype(F32))
        red = red + through * tile[0:8]
        green = green + through * tile[8:16]
        blue = blue + through * tile[16:24]
        return (through * (1.0 - tile[24:32]), red, green, blue)

    zero = jnp.zeros((8, cols), F32)
    through, red, green, blue = lax.fori_loop(
        0, slabs, body, (jnp.ones((8, cols), F32), zero, zero, zero), unroll=8
    )
    image_ref[0] = red
    image_ref[1] = green
    image_ref[2] = blue
    image_ref[3] = 1.0 - through
    last = pltpu.make_async_copy(image_ref, far_ref, sems.at[1])
    last.start()
    copy.wait()
    last.wait()


def compose(parts, flag, mean):
    return pl.pallas_call(
        compose_kernel,
        out_shape=(
            jax.ShapeDtypeStruct((4, 8, parts.shape[2]), F32),
            jax.ShapeDtypeStruct(mean.shape, F32),
        ),
        in_specs=[VMEM, SMEM, VMEM],
        out_specs=(pl.BlockSpec(memory_space=pltpu.HBM),) * 2,
        scratch_shapes=[
            pltpu.VMEM((4, 8, parts.shape[2]), F32),
            pltpu.SemaphoreType.DMA((2,)),
        ],
        compiler_params=GRANT,
        name="compose",
    )(near(parts), pltpu.with_memory_space_constraint(flag, pltpu.SMEM), near(mean))


def mates(count, start):
    low = range(start, count - 1, 2)
    return [(i, i + 1) for i in low] + [(i + 1, i) for i in low]


def shards(coarse, residual, levels, slab_rank, light_angles, color_slope, color_shift):
    dep = residual.shape[0]
    slabs, tiles = lax.axis_size("depth"), lax.axis_size("tile")
    step = 4.0 / (dep * slabs)
    full, z1, z2 = refine(residual, coarse, levels)
    x1, x2 = columns(full)
    z1 = lax.ppermute(z1, "depth", mates(slabs, 1))
    z2 = lax.ppermute(z2, "depth", mates(slabs, 0))
    x1 = lax.ppermute(x1, "tile", mates(tiles, 0))
    x2 = lax.ppermute(x2, "tile", mates(tiles, 1))
    *ready, gx, forward = prepare(step, full, slab_rank, light_angles, color_slope, color_shift)
    ready[:2] = mend(*ready[:2], gx, ready[-1], x1, x2)
    image, mean = shade(z1, z2, ready)
    order = sorted(range(slabs), key=seat)
    parts = lax.all_to_all(
        image, "depth", split_axis=0, concat_axis=0, tiled=True, axis_index_groups=[order]
    )
    return compose(parts, forward, mean)


def solution(mesh):
    placed = (
        P("depth", None, "tile"),
        P("depth", None, "tile"),
        P("depth", None, "tile"),
        P(),
        P(),
        P(),
        P(),
    )
    return jax.shard_map(
        shards,
        mesh=mesh,
        in_specs=placed,
        out_specs=(P(None, "depth", "tile"), P("depth", None, "tile")),
        check_vma=False,
    )
```
